32 devices in a mesh: sp: 8 (over z, y), tp: 4 (over x, core).
Axes of the slice: x: 2, y: 2, z: 4, core: 2. Of those that a mesh axis runs over, the one named last changes fastest.
Arguments:
- decay_rate: float32 [1, 4096, 4096], P(None, 'sp', 'tp'), may hold values from 0.2 to 2
- drive_in: bfloat16 [1, 4096, 4096], P(None, 'sp', 'tp'), may hold values from -6 to 6
- gate_in: bfloat16 [1, 4096, 4096], P(None, 'sp', 'tp'), may hold values from -6 to 6
- norm_gain: float32 [4096], P('tp'), may hold values from 0.25 to 1.75
Outputs:
- filtered: bfloat16 [1, 4096, 4096], P(None, 'sp', 'tp')
The draws below stay inside these ranges and needn't reach their ends.
All inputs are finite; a program needn't handle non-finite values.
Results may differ from the reference program's by a relative error of at most 0.001.
Values sent between devices are 32-bit elements; how exact they have to be, the bound alone decides.
A program may use at most 64 MiB of HBM per device.

```python
import jax
import jax.numpy as jnp
from jax import lax

BATCH = 1
CHANNELS = 4096
LENGTH = 4096


def block_levels(key, extent, cuts, smallest, largest):
    def one(dim, shards_of):
        steps = jax.random.uniform(jax.random.fold_in(jax.random.fold_in(key, 6), dim), (shards_of,), jnp.float32, smallest / len(cuts), largest / len(cuts))
        return jnp.repeat(jnp.exp(steps), extent[dim] // shards_of).reshape((-1,) + (1,) * (len(extent) - dim - 1))

    loudness = one(*cuts[0])
    for cut in cuts[1:]:
        loudness = loudness * one(*cut)
    return loudness


def scatter_about(own_key, shape, width, reach, shards=(), held_as=jnp.bfloat16):
    entries = jax.random.normal(own_key, shape, jnp.float32) * width
    if len(shards) > 0:
        entries = block_levels(own_key, shape, shards, -0.22, 0.18) * entries
    return jnp.clip(entries, min=-reach, max=reach).astype(held_as)


def setup_inputs(seed: int = 0) -> dict:
    key_list = jax.random.split(jax.random.key(seed), 5)
    decay_rate = jnp.clip(0.2 + 1.8 * jax.random.uniform(key_list[0], (BATCH, LENGTH, CHANNELS), jnp.float32) ** block_levels(key_list[0], (BATCH, LENGTH, CHANNELS), ((1, 8), (2, 4)), -0.2, 0.2), 0.2, 2.0)
    drive_in = scatter_about(key_list[1], (BATCH, LENGTH, CHANNELS), 1.0, 6.0, ((1, 8), (2, 4)))
    gate_in = scatter_about(key_list[2], (BATCH, LENGTH, CHANNELS), 1.0, 6.0, ((1, 8), (2, 4)))
    norm_gain = jnp.clip(1.0 + 0.15 * jax.random.normal(key_list[3], (CHANNELS,), jnp.float32), 0.25, 1.75)
    return {"decay_rate": decay_rate, "drive_in": drive_in, "gate_in": gate_in, "norm_gain": norm_gain}


def join_pair(earlier, later):
    return (earlier[0] * later[0], later[0] * earlier[1] + later[1])

def reference(decay_rate, drive_in, gate_in, norm_gain):
    keep = jnp.exp(-decay_rate / LENGTH)
    push = drive_in.astype(jnp.float32) * LENGTH ** (-0.5)
    forward = lax.associative_scan(join_pair, (keep, push), axis=1)[1]
    backward = lax.associative_scan(join_pair, (keep, push), axis=1, reverse=True)[1]
    states = forward + backward
    gated = states * jax.nn.sigmoid(gate_in.astype(jnp.float32))
    power = lax.optimization_barrier(jnp.mean(gated * gated, axis=-1, keepdims=True))
    filtered = (gated * lax.rsqrt(power + 1e-06) * norm_gain).astype(jnp.bfloat16)
    return filtered
```

```python
import functools

import jax
import jax.numpy as jnp
from jax import lax
from jax.experimental import pallas as pl
from jax.experimental.pallas import tpu as pltpu
from jax.sharding import PartitionSpec as P

LANES = 128
SUB = 8
LOG2E = 1.4426950408889634
MESH = pl.DeviceIdType.MESH


def spaced(steps):
    return steps + next(more for more in range(4, 40, 4) if (steps + more) % 8 == 4)


def strands(steps):
    return next(size for size in (4, 2, 1) if steps % size == 0)


def kernel(
    nsp, ntp, decay, drive, gate, gain, gated, inverse,
    decay_v, drive_v, gate_v, decay_s, push_s, sig_s, fwd_s, pre_s, base_s, left_s, right_s,
    part_s, ends_s, edge_s, enter_s, totals, powers, gain_v,
    gain_sem, in_sem, tsend, trecv, psend, precv,
):
    rows, channels = decay.shape
    tiles = channels // LANES
    steps = rows // SUB
    length = rows * nsp
    pitch = spaced(steps)
    high = strands(steps)
    run = steps // high
    near = spaced(max(SUB, tiles))
    me, mine = lax.axis_index("sp"), lax.axis_index("tp")

    sources = ((decay, decay_v), (drive, drive_v), (gate, gate_v))

    def load(kind, j):
        source, held = sources[kind]
        lanes = pl.ds(pl.multiple_of(j * LANES, LANES), LANES)
        return pltpu.make_async_copy(source.at[:, lanes], held.at[j], in_sem.at[kind, j])

    for j in range(tiles):
        load(0, j).start()
        load(1, j).start()

    barrier = pltpu.get_barrier_semaphore()

    def peers():
        ahead_first = (2 * me + 1) // nsp
        for i in range(nsp - 1):
            up = nsp - 1 - i - (i + me + 1) // nsp
            down = i + (nsp - 1 - me + i + 1) // nsp
            yield up * (1 - ahead_first) + down * ahead_first

    for peer in peers():
        pl.semaphore_signal(barrier, inc=1, device_id={"sp": peer}, device_id_type=MESH)
    for d in range(1, ntp):
        pl.semaphore_signal(barrier, inc=1, device_id={"tp": lax.rem(mine + d, ntp)}, device_id_type=MESH)

    for j in range(tiles):
        load(2, j).start()
    gain_copy = pltpu.make_async_copy(gain, gain_v, gain_sem)
    gain_copy.start()

    zero = jnp.zeros((SUB, LANES), jnp.float32)
    one = jnp.ones((SUB, LANES), jnp.float32)

    def at(k):
        return pl.ds(k, SUB, stride=pitch)

    chunks = [(pl.ds(i * steps, steps), pl.ds(i * pitch, steps)) for i in range(SUB)]

    def scan(j, carry):
        load(0, j).wait()
        for dense, apart in chunks:
            decay_s[j, apart, :] = jnp.exp2(decay_v[j, dense, :] * (-LOG2E / length))
        load(1, j).wait()
        for dense, apart in chunks:
            push_s[j, apart, :] = drive_v[j, dense, :].astype(jnp.float32)
        prod, fwd, bwd = [one] * high, [zero] * high, [zero] * high
        for k in range(run):
            for h in range(high):
                t = h * run + k
                keep = decay_s[j, at(t), :]
                push = push_s[j, at(t), :]
                if k == 0:
                    bwd[h], prod[h], fwd[h] = push, keep, push
                else:
                    bwd[h] = bwd[h] + prod[h] * push
                    prod[h] = prod[h] * keep
                    fwd[h] = keep * fwd[h] + push
                fwd_s[j, pl.ds(t * SUB, SUB), :] = fwd[h]
                pre_s[j, pl.ds(t * SUB, SUB), :] = prod[h]
        for h in range(high):
            part_s[j, 0, h] = prod[h]
            part_s[j, 1, h] = fwd[h]
            part_s[j, 2, h] = bwd[h]
        whole, first, last = prod[0], fwd[0], bwd[high - 1]
        for h in range(1, high):
            first = prod[h] * first + fwd[h]
            whole = whole * prod[h]
            e = high - 1 - h
            last = prod[e] * last + bwd[e]
        for q, value in enumerate((whole, first, last)):
            ends_s[q, pl.ds(j * near, SUB), :] = value
        return carry

    lax.fori_loop(0, tiles, scan, 0)

    def chunk(q, i):
        return ends_s[q, pl.ds(i, tiles, stride=near), :]

    whole = [chunk(0, i) for i in range(SUB)]
    first = [chunk(1, i) for i in range(SUB)]
    last = [chunk(2, i) for i in range(SUB)]
    ups, downs = [], []
    pp, pf = jnp.ones((tiles, LANES), jnp.float32), jnp.zeros((tiles, LANES), jnp.float32)
    qp, qb = pp, pf
    for i in range(SUB):
        ups.append((pp, pf))
        pf = whole[i] * pf + first[i]
        pp = pp * whole[i]
        e = SUB - 1 - i
        downs.append((qp, qb))
        qb = whole[e] * qb + last[e]
        qp = qp * whole[e]
    totals[me, 0] = qb
    totals[me, 1] = pp
    totals[me, 2] = pf

    pl.semaphore_wait(barrier, nsp + ntp - 2)

    def share(peer, d):
        part = pl.ds(1 - (me + d) // nsp, 2)
        return pltpu.make_async_remote_copy(
            src_ref=totals.at[me, part],
            dst_ref=totals.at[me, part],
            send_sem=tsend.at[d],
            recv_sem=trecv.at[d],
            device_id={"sp": peer},
            device_id_type=MESH,
        )

    sends = [share(peer, lax.rem(peer - me + nsp, nsp)) for peer in peers()]
    for copy in sends:
        copy.start()

    for i in range(SUB):
        spot = pl.ds(i * near, tiles)
        edge_s[0, spot, :], edge_s[1, spot, :] = ups[i]
        edge_s[2, spot, :], edge_s[3, spot, :] = downs[SUB - 1 - i]

    def gates(j, carry):
        load(2, j).wait()
        for dense, apart in chunks:
            value = gate_v[j, dense, :].astype(jnp.float32)
            sig_s[j, apart, :] = 1.0 / (1.0 + jnp.exp2(value * -LOG2E))
        prod = [part_s[j, 0, h] for h in range(high)]
        fwd = [part_s[j, 1, h] for h in range(high)]
        bwd = [part_s[j, 2, h] for h in range(high)]
        pp, pf, qp, qb = (edge_s[q, pl.ds(j, SUB, stride=near), :] for q in range(4))
        enter, span, suf, back = [], [], [None] * high, [None] * high
        for h in range(high):
            enter.append(pf)
            span.append(pp)
            pf = prod[h] * pf + fwd[h]
            pp = pp * prod[h]
        for h in reversed(range(high)):
            suf[h], back[h] = qp, qb
            qb = prod[h] * qb + bwd[h]
            qp = qp * prod[h]
        for k in reversed(range(run)):
            for h in range(high):
                t = h * run + k
                keep = decay_s[j, at(t), :]
                sig = sig_s[j, at(t), :]
                back[h] = keep * back[h] + push_s[j, at(t), :]
                suf[h] = keep * suf[h]
                lead = pre_s[j, pl.ds(t * SUB, SUB), :] * sig
                base_s[j, at(t), :] = (fwd_s[j, pl.ds(t * SUB, SUB), :] + back[h]) * sig + lead * enter[h]
                left_s[j, at(t), :] = lead * span[h]
                right_s[j, at(t), :] = suf[h] * sig
        return carry

    lax.fori_loop(0, tiles, gates, 0)

    def arrive(n, carry):
        share(me, carry - n).wait_recv()
        return carry

    def spread(q, j):
        return jnp.broadcast_to(enter_s[q, pl.ds(j, 1), :], (SUB, LANES))

    lax.fori_loop(0, me, arrive, me)

    def join(s, enter):
        return totals[s, 1] * enter + totals[s, 2]

    enter_s[0] = lax.fori_loop(0, me, join, jnp.zeros((tiles, LANES), jnp.float32))

    spots = [i * pitch + r for i in range(SUB) for r in range(0, steps, SUB)]

    def settle(j, carry):
        enter = spread(0, j)
        for spot in spots:
            spot = pl.ds(spot, SUB)
            base_s[j, spot, :] = base_s[j, spot, :] + left_s[j, spot, :] * enter
        return carry

    lax.fori_loop(0, tiles, settle, 0)

    lax.fori_loop(0, nsp - 1 - me, arrive, nsp - 1)

    enter = jnp.zeros((tiles, LANES), jnp.float32)
    for s in range(nsp - 1):
        e = nsp - 1 - s
        enter = jnp.where(e > me, totals[e, 1] * enter + totals[e, 0], enter)
    enter_s[1] = enter

    width = powers.shape[-1]
    lane = lax.broadcasted_iota(jnp.int32, (SUB, width), 1)
    enters = [spread(1, j) for j in range(tiles)]
    sums = jnp.zeros((SUB, width), jnp.float32)
    for g, spot in enumerate(spots):
        spot = pl.ds(spot, SUB)
        squares = zero
        for j in range(tiles):
            value = base_s[j, spot, :] + right_s[j, spot, :] * enters[j]
            squares = squares + value * value
        sums = jnp.where(lane == g, jnp.sum(squares, axis=1, keepdims=True), sums)
    powers[mine] = sums

    tells = []
    for d in sorted(range(1, ntp), key=lambda d: abs(2 * d - ntp)):
        tells.append(pltpu.make_async_remote_copy(
            src_ref=powers.at[mine],
            dst_ref=powers.at[mine],
            send_sem=psend.at[d],
            recv_sem=precv.at[d],
            device_id={"tp": lax.rem(mine + d, ntp)},
            device_id_type=MESH,
        ))
    for copy in tells:
        copy.start()
    gain_copy.wait()

    def weigh(j, carry):
        own = jnp.broadcast_to(gain_v[pl.ds(j, 1), :], (SUB, LANES))
        enter = spread(1, j)
        for g, spot in enumerate(spots):
            spot = pl.ds(spot, SUB)
            gated[j, pl.ds(g * SUB, SUB), :] = (base_s[j, spot, :] + right_s[j, spot, :] * enter) * own
        return carry

    lax.fori_loop(0, tiles, weigh, 0)

    for copy in sends:
        copy.wait_send()
    for copy in tells:
        copy.wait()

    power = powers[0]
    for s in range(1, ntp):
        power = power + powers[s]
    power = power * (1.0 / (length * channels * ntp))
    inverse[...] = lax.rsqrt(power + 1e-06) * length ** (-0.5)


def emit(gated, inverse, out, staged, sems):
    rows, channels = out.shape
    tiles = channels // LANES
    pair = 2 * SUB
    block = rows // SUB
    scale = inverse[...]
    copies = []
    for b in range(SUB):
        for row in range(b * block, (b + 1) * block, pair):
            g = row // SUB
            own = jnp.concatenate([
                jnp.broadcast_to(scale[:, g + n : g + n + 1], (SUB, LANES)) for n in range(2)
            ], axis=0)
            for j in range(tiles):
                staged[pl.ds(row, pair), pl.ds(j * LANES, LANES)] = (
                    gated[j, pl.ds(row, pair), :] * own
                ).astype(jnp.bfloat16)
        dense = pl.ds(b * block, block)
        copies.append(pltpu.make_async_copy(staged.at[dense], out.at[dense], sems.at[b]))
        copies[-1].start()
    for copy in copies:
        copy.wait()


def body(nsp, ntp, decay_rate, drive_in, gate_in, norm_gain):
    batch, rows, channels = decay_rate.shape
    tiles = channels // LANES
    steps = rows // SUB
    high = strands(steps)
    near = spaced(max(SUB, tiles))
    width = -(-steps // LANES) * LANES
    plane = pltpu.VMEM((tiles, rows, LANES), jnp.float32)
    wide = pltpu.VMEM((tiles, SUB * spaced(steps), LANES), jnp.float32)
    half = pltpu.VMEM((tiles, rows, LANES), jnp.bfloat16)
    outside = pl.BlockSpec(memory_space=pltpu.HBM)
    vmem = pl.BlockSpec(memory_space=pltpu.VMEM)
    gated, inverse = pl.pallas_call(
        functools.partial(kernel, nsp, ntp),
        out_shape=(
            pltpu.VMEM((tiles, rows, LANES), jnp.float32),
            pltpu.VMEM((SUB, width), jnp.float32),
        ),
        in_specs=[outside] * 4,
        out_specs=(vmem, vmem),
        scratch_shapes=[
            plane, half, half, wide, wide, wide, plane, plane, wide, wide, wide,
            pltpu.VMEM((tiles, 3, high, SUB, LANES), jnp.float32),
            pltpu.VMEM((3, tiles * near, LANES), jnp.float32),
            pltpu.VMEM((4, SUB * near, LANES), jnp.float32),
            pltpu.VMEM((2, tiles, LANES), jnp.float32),
            pltpu.VMEM((nsp, 3, tiles, LANES), jnp.float32),
            pltpu.VMEM((ntp, SUB, width), jnp.float32),
            pltpu.VMEM((tiles, LANES), jnp.float32),
            pltpu.SemaphoreType.DMA,
            pltpu.SemaphoreType.DMA((3, tiles)),
            pltpu.SemaphoreType.DMA((nsp,)),
            pltpu.SemaphoreType.DMA((nsp,)),
            pltpu.SemaphoreType.DMA((ntp,)),
            pltpu.SemaphoreType.DMA((ntp,)),
        ],
        compiler_params=pltpu.CompilerParams(
            collective_id=0, has_side_effects=True, vmem_limit_bytes=52 * 1024 * 1024
        ),
    )(*(
        pltpu.with_memory_space_constraint(value, pltpu.HBM)
        for value in (
            decay_rate.reshape(rows, channels),
            drive_in.reshape(rows, channels),
            gate_in.reshape(rows, channels),
            norm_gain.reshape(tiles, LANES),
        )
    ))
    result = pl.pallas_call(
        emit,
        out_shape=jax.ShapeDtypeStruct((rows, channels), jnp.bfloat16),
        in_specs=[vmem, vmem],
        out_specs=outside,
        scratch_shapes=[
            pltpu.VMEM((rows, channels), jnp.bfloat16),
            pltpu.SemaphoreType.DMA((SUB,)),
        ],
        compiler_params=pltpu.CompilerParams(vmem_limit_bytes=32 * 1024 * 1024),
    )(
        pltpu.with_memory_space_constraint(gated, pltpu.VMEM),
        pltpu.with_memory_space_constraint(inverse, pltpu.VMEM),
    )
    return result.reshape(batch, rows, channels)


def solution(mesh):
    in_specs = (P(None, "sp", "tp"), P(None, "sp", "tp"), P(None, "sp", "tp"), P("tp"))
    out_specs = P(None, "sp", "tp")
    local = functools.partial(body, mesh.shape["sp"], mesh.shape["tp"])
    return jax.shard_map(local, mesh=mesh, in_specs=in_specs, out_specs=out_specs, check_vma=False)
```

```python
import functools

import jax
import jax.numpy as jnp
from jax import lax
from jax.experimental import pallas as pl
from jax.experimental.pallas import tpu as pltpu
from jax.sharding import PartitionSpec as P

LANES = 128
SUB = 8
LOG2E = 1.4426950408889634
MESH = pl.DeviceIdType.MESH


def spaced(steps):
    return steps + next(more for more in range(4, 40, 4) if (steps + more) % 8 == 4)


def strands(steps):
    return next(size for size in (4, 2, 1) if steps % size == 0)


def reduced(spans):
    while len(spans) > 1:
        spans = [
            (p * q, q * f + g, b + p * c) for (p, f, b), (q, g, c) in zip(spans[::2], spans[1::2])
        ] + spans[len(spans) - len(spans) % 2 :]
    return spans[0]


def kernel(
    nsp, ntp, decay, drive, gate, gain, gated, inverse,
    decay_v, drive_v, gate_v, decay_s, push_s, sig_s, fwd_s, pre_s, base_s, left_s, right_s,
    part_s, ends_s, edge_s, enter_s, totals, powers, gain_v, local, trecv, precv,
):
    rows, channels = decay.shape
    tiles = channels // LANES
    steps = rows // SUB
    length = rows * nsp
    pitch = spaced(steps)
    high = strands(steps)
    run = steps // high
    near = spaced(max(SUB, tiles))
    me, mine = lax.axis_index("sp"), lax.axis_index("tp")

    final = tiles - 1

    def load(source, held, j, sem):
        lanes = pl.ds(j * LANES, LANES)
        pltpu.make_async_copy(source.at[:, lanes], held.at[j], local.at[sem]).start()

    def drain(ref, sem):
        pltpu.make_async_copy(ref, ref, sem).wait()

    for j in range(tiles):
        load(decay, decay_v, j, j)
        load(drive, drive_v, j, j if j < final else tiles)

    barrier = pltpu.get_barrier_semaphore()

    def peers():
        ahead_first = (2 * me + 1) // nsp
        for i in range(nsp - 1):
            up = nsp - 1 - i - (i + me + 1) // nsp
            down = i + (nsp - 1 - me + i + 1) // nsp
            yield up * (1 - ahead_first) + down * ahead_first

    for peer in peers():
        pl.semaphore_signal(barrier, inc=1, device_id={"sp": peer}, device_id_type=MESH)
    for d in range(1, ntp):
        pl.semaphore_signal(barrier, inc=1, device_id={"tp": lax.rem(mine + d, ntp)}, device_id_type=MESH)

    zero = jnp.zeros((SUB, LANES), jnp.float32)
    one = jnp.ones((SUB, LANES), jnp.float32)

    def at(k):
        return pl.ds(k, SUB, stride=pitch)

    chunks = [(pl.ds(i * steps, steps), pl.ds(i * pitch, steps)) for i in range(SUB)]

    def scan(j, carry):
        if isinstance(j, int):
            drain(decay_v.at[j], local.at[j])
        else:
            drain(fwd_s.at[pl.ds(0, 3), pl.ds(0, rows // 2)], local.at[j])
        for dense, apart in chunks:
            decay_s[j, apart, :] = jnp.exp2(decay_v[j, dense, :] * (-LOG2E / length))
        if isinstance(j, int):
            drain(drive_v.at[j], local.at[tiles])
        for dense, apart in chunks:
            push_s[j, apart, :] = drive_v[j, dense, :].astype(jnp.float32)
        prod, fwd, bwd = [one] * high, [zero] * high, [zero] * high
        for k in range(run):
            for h in range(high):
                t = h * run + k
                keep = decay_s[j, at(t), :]
                push = push_s[j, at(t), :]
                if k == 0:
                    bwd[h], prod[h], fwd[h] = push, keep, push
                else:
                    bwd[h] = bwd[h] + prod[h] * push
                    prod[h] = prod[h] * keep
                    fwd[h] = keep * fwd[h] + push
                fwd_s[j, pl.ds(t * SUB, SUB), :] = fwd[h]
                pre_s[j, pl.ds(t * SUB, SUB), :] = prod[h]
        for h in range(high):
            part_s[j, 0, h] = prod[h]
            part_s[j, 1, h] = fwd[h]
            part_s[j, 2, h] = bwd[h]
        for q, value in enumerate(reduced(list(zip(prod, fwd, bwd)))):
            ends_s[q, pl.ds(j * near, SUB), :] = value
        return carry

    lax.fori_loop(0, final, scan, 0)
    for j in range(tiles):
        load(gate, gate_v, j, 0)
    pltpu.make_async_copy(gain, gain_v, local.at[1]).start()
    scan(final, 0)

    def chunk(q, i):
        return ends_s[q, pl.ds(i, tiles, stride=near), :]

    whole = [chunk(0, i) for i in range(SUB)]
    first = [chunk(1, i) for i in range(SUB)]
    last = [chunk(2, i) for i in range(SUB)]
    totals[me, 1], totals[me, 2], totals[me, 0] = reduced(list(zip(whole, first, last)))

    pl.semaphore_wait(barrier, nsp + ntp - 2)

    def share(peer, d):
        part = pl.ds(1 - (me + d) // nsp, 2)
        return pltpu.make_async_remote_copy(
            src_ref=totals.at[me, part],
            dst_ref=totals.at[me, part],
            send_sem=local.at[2],
            recv_sem=trecv.at[d - 1],
            device_id={"sp": peer},
            device_id_type=MESH,
        )

    sends = [share(peer, lax.rem(peer - me + nsp, nsp)) for peer in peers()]
    for copy in sends:
        copy.start()

    pp, pf = jnp.ones((tiles, LANES), jnp.float32), jnp.zeros((tiles, LANES), jnp.float32)
    qp, qb = pp, pf
    for i in range(SUB):
        e = SUB - 1 - i
        edge_s[0, pl.ds(i * near, tiles), :], edge_s[1, pl.ds(i * near, tiles), :] = pp, pf
        edge_s[2, pl.ds(e * near, tiles), :], edge_s[3, pl.ds(e * near, tiles), :] = qp, qb
        pf = whole[i] * pf + first[i]
        pp = pp * whole[i]
        qb = whole[e] * qb + last[e]
        qp = qp * whole[e]

    drain(gate_v, local.at[0])

    def gates(j, carry):
        for dense, apart in chunks:
            value = gate_v[j, dense, :].astype(jnp.float32)
            sig_s[j, apart, :] = 1.0 / (1.0 + jnp.exp2(value * -LOG2E))
        prod = [part_s[j, 0, h] for h in range(high)]
        fwd = [part_s[j, 1, h] for h in range(high)]
        bwd = [part_s[j, 2, h] for h in range(high)]
        pp, pf, qp, qb = (edge_s[q, pl.ds(j, SUB, stride=near), :] for q in range(4))
        enter, span, suf, back = [], [], [None] * high, [None] * high
        for h in range(high):
            enter.append(pf)
            span.append(pp)
            pf = prod[h] * pf + fwd[h]
            pp = pp * prod[h]
        for h in reversed(range(high)):
            suf[h], back[h] = qp, qb
            qb = prod[h] * qb + bwd[h]
            qp = qp * prod[h]
        for k in reversed(range(run)):
            for h in range(high):
                t = h * run + k
                keep = decay_s[j, at(t), :]
                sig = sig_s[j, at(t), :]
                back[h] = keep * back[h] + push_s[j, at(t), :]
                suf[h] = keep * suf[h]
                lead = pre_s[j, pl.ds(t * SUB, SUB), :] * sig
                base_s[j, at(t), :] = (fwd_s[j, pl.ds(t * SUB, SUB), :] + back[h]) * sig + lead * enter[h]
                left_s[j, at(t), :] = lead * span[h]
                right_s[j, at(t), :] = suf[h] * sig
        return carry

    lax.fori_loop(0, tiles, gates, 0)

    def arrive(n, carry):
        share(me, carry - n).wait_recv()
        return carry

    def spread(q, j):
        return jnp.broadcast_to(enter_s[q, pl.ds(j, 1), :], (SUB, LANES))

    lax.fori_loop(0, me, arrive, me)

    def join(s, enter):
        return totals[s, 1] * enter + totals[s, 2]

    enter_s[0] = lax.fori_loop(0, me, join, jnp.zeros((tiles, LANES), jnp.float32))

    spots = [i * pitch + r for i in range(SUB) for r in range(0, steps, SUB)]

    def settle(j, carry):
        enter = spread(0, j)
        for spot in spots:
            spot = pl.ds(spot, SUB)
            base_s[j, spot, :] = base_s[j, spot, :] + left_s[j, spot, :] * enter
        return carry

    lax.fori_loop(0, tiles, settle, 0)

    lax.fori_loop(0, nsp - 2 - me, arrive, nsp - 1)

    def prepend(n, carry):
        enter, span = carry
        e = me + 1 + n
        return enter + span * totals[e, 0], span * totals[e, 1]

    blank = jnp.zeros((tiles, LANES), jnp.float32)
    enter, span = lax.fori_loop(0, nsp - 2 - me, prepend, (blank, blank + 1.0))
    enter_s[1] = enter
    enter_s[2] = jnp.where(me < nsp - 1, span, 0.0)
    enters = [(spread(1, j), spread(2, j)) for j in range(tiles)]

    @pl.when(me < nsp - 1)
    def _():
        share(me, me + 1).wait_recv()

    enters = [
        enter + span * jnp.broadcast_to(totals[nsp - 1, 0, pl.ds(j, 1), :], (SUB, LANES))
        for j, (enter, span) in enumerate(enters)
    ]
    width = powers.shape[-1]
    lane = lax.broadcasted_iota(jnp.int32, (SUB, width), 1)
    sums = jnp.zeros((SUB, width), jnp.float32)
    for g, spot in enumerate(spots):
        spot = pl.ds(spot, SUB)
        squares = zero
        for j in range(tiles):
            value = base_s[j, spot, :] + right_s[j, spot, :] * enters[j]
            squares = squares + value * value
        sums = jnp.where(lane == g, jnp.sum(squares, axis=1, keepdims=True), sums)
    powers[mine] = sums

    tells = []
    for d in sorted(range(1, ntp), key=lambda d: abs(2 * d - ntp)):
        tells.append(pltpu.make_async_remote_copy(
            src_ref=powers.at[mine],
            dst_ref=powers.at[mine],
            send_sem=local.at[3],
            recv_sem=precv,
            device_id={"tp": lax.rem(mine + d, ntp)},
            device_id_type=MESH,
        ))
    for copy in tells:
        copy.start()
    enter_s[1] = enter_s[1] + enter_s[2] * totals[nsp - 1, 0]
    drain(gain_v, local.at[1])

    def weigh(j, carry):
        own = jnp.broadcast_to(gain_v[pl.ds(j, 1), :], (SUB, LANES))
        enter = spread(1, j)
        for g, spot in enumerate(spots):
            spot = pl.ds(spot, SUB)
            gated[j, pl.ds(g * SUB, SUB), :] = (base_s[j, spot, :] + right_s[j, spot, :] * enter) * own
        return carry

    lax.fori_loop(0, tiles, weigh, 0)

    drain(totals.at[pl.ds(0, nsp - 1), pl.ds(0, 2)], local.at[2])
    drain(powers.at[pl.ds(0, ntp - 1)], local.at[3])
    drain(powers.at[pl.ds(0, ntp - 1)], precv)

    power = powers[0]
    for s in range(1, ntp):
        power = power + powers[s]
    power = power * (1.0 / (length * channels * ntp))
    inverse[...] = lax.rsqrt(power + 1e-06) * length ** (-0.5)


def emit(gated, inverse, out, staged, sem):
    rows, channels = out.shape
    tiles = channels // LANES
    pair = 2 * SUB
    block = rows // SUB
    scale = inverse[...]
    for b in range(SUB):
        for row in range(b * block, (b + 1) * block, pair):
            g = row // SUB
            own = jnp.concatenate([
                jnp.broadcast_to(scale[:, g + n : g + n + 1], (SUB, LANES)) for n in range(2)
            ], axis=0)
            for j in range(tiles):
                staged[pl.ds(row, pair), pl.ds(j * LANES, LANES)] = (
                    gated[j, pl.ds(row, pair), :] * own
                ).astype(jnp.bfloat16)
        dense = pl.ds(b * block, block)
        pltpu.make_async_copy(staged.at[dense], out.at[dense], sem).start()
    pltpu.make_async_copy(staged, out, sem).wait()


def body(nsp, ntp, decay_rate, drive_in, gate_in, norm_gain):
    batch, rows, channels = decay_rate.shape
    tiles = channels // LANES
    steps = rows // SUB
    high = strands(steps)
    near = spaced(max(SUB, tiles))
    width = -(-steps // LANES) * LANES
    plane = pltpu.VMEM((tiles, rows, LANES), jnp.float32)
    wide = pltpu.VMEM((tiles, SUB * spaced(steps) + SUB, LANES), jnp.float32)
    half = pltpu.VMEM((tiles, rows, LANES), jnp.bfloat16)
    outside = pl.BlockSpec(memory_space=pltpu.HBM)
    vmem = pl.BlockSpec(memory_space=pltpu.VMEM)
    gated, inverse = pl.pallas_call(
        functools.partial(kernel, nsp, ntp),
        out_shape=(
            pltpu.VMEM((tiles, rows, LANES), jnp.float32),
            pltpu.VMEM((SUB, width), jnp.float32),
        ),
        in_specs=[outside] * 4,
        out_specs=(vmem, vmem),
        scratch_shapes=[
            plane, half, half, wide, wide, wide, plane, plane, wide, wide, wide,
            pltpu.VMEM((tiles, 3, high, SUB, LANES), jnp.float32),
            pltpu.VMEM((3, tiles * near, LANES), jnp.float32),
            pltpu.VMEM((4, SUB * near, LANES), jnp.float32),
            pltpu.VMEM((3, tiles, LANES), jnp.float32),
            pltpu.VMEM((nsp, 3, tiles, LANES), jnp.float32),
            pltpu.VMEM((ntp, SUB, width), jnp.float32),
            pltpu.VMEM((tiles, LANES), jnp.float32),
            pltpu.SemaphoreType.DMA((max(tiles + 1, 4),)),
            pltpu.SemaphoreType.DMA((nsp - 1,)),
            pltpu.SemaphoreType.DMA,
        ],
        compiler_params=pltpu.CompilerParams(
            collective_id=0, has_side_effects=True, vmem_limit_bytes=52 * 1024 * 1024
        ),
    )(*(
        pltpu.with_memory_space_constraint(value, pltpu.HBM)
        for value in (
            decay_rate.reshape(rows, channels),
            drive_in.reshape(rows, channels),
            gate_in.reshape(rows, channels),
            norm_gain.reshape(tiles, LANES),
        )
    ))
    result = pl.pallas_call(
        emit,
        out_shape=jax.ShapeDtypeStruct((rows, channels), jnp.bfloat16),
        in_specs=[vmem, vmem],
        out_specs=outside,
        scratch_shapes=[
            pltpu.VMEM((rows, channels), jnp.bfloat16),
            pltpu.SemaphoreType.DMA,
        ],
        compiler_params=pltpu.CompilerParams(vmem_limit_bytes=32 * 1024 * 1024),
    )(
        pltpu.with_memory_space_constraint(gated, pltpu.VMEM),
        pltpu.with_memory_space_constraint(inverse, pltpu.VMEM),
    )
    return result.reshape(batch, rows, channels)


def solution(mesh):
    in_specs = (P(None, "sp", "tp"), P(None, "sp", "tp"), P(None, "sp", "tp"), P("tp"))
    out_specs = P(None, "sp", "tp")
    local = functools.partial(body, mesh.shape["sp"], mesh.shape["tp"])
    return jax.shard_map(local, mesh=mesh, in_specs=in_specs, out_specs=out_specs, check_vma=False)
```

```python
import functools

import jax
import jax.numpy as jnp
from jax import lax
from jax.experimental import pallas as pl
from jax.experimental.pallas import tpu as pltpu
from jax.sharding import PartitionSpec as P

LANES = 128
SUB = 8
LOG2E = 1.4426950408889634
MESH = pl.DeviceIdType.MESH


def spaced(steps):
    return steps + next(more for more in range(4, 40, 4) if (steps + more) % 8 == 4)


PITCH = spaced(SUB)
UNIT = SUB * SUB
APART = SUB * PITCH + 1
PUSH, SIG, LEFT, RIGHT = 2, 1, 1, 8


def joined(early, late):
    (p, f, b), (q, g, c) = early, late
    return p * q, q * f + g, b + p * c


def reduced(spans):
    while len(spans) > 1:
        spans = [joined(*pair) for pair in zip(spans[::2], spans[1::2])] + spans[len(spans) - len(spans) % 2 :]
    return spans[0]


def blocked(units):
    return [range(u, u + 2) for u in range(0, units - 2, 2)] + [range(u, u + 1) for u in range(units - 2 + units % 2, units)]


def kernel(
    nsp, ntp, decay, drive, gate, gain, gated, inverse,
    decay_v, drive_v, gate_v, decay_s, push_s, sig_s, fwd_s, pre_s, base_s, left_s, right_s,
    ends_s, edge_s, enter_s, totals, powers, gain_v, local, trecv, precv,
):
    rows, channels = decay.shape
    tiles = channels // LANES
    units = rows // UNIT
    groups = rows // SUB
    length = rows * nsp
    near = spaced(max(SUB, tiles))
    me, mine = lax.axis_index("sp"), lax.axis_index("tp")
    blocks = blocked(units)
    final = len(blocks) - 1

    def band(block):
        return pl.ds(block[0] * UNIT, len(block) * UNIT)

    def drain(ref, sem):
        pltpu.make_async_copy(ref, ref, sem).wait()

    for n, block in enumerate(blocks):
        pltpu.make_async_copy(decay.at[band(block)], decay_v.at[band(block)], local.at[n]).start()
        pltpu.make_async_copy(
            drive.at[band(block)], drive_v.at[band(block)], local.at[n if n < final else n + 1]
        ).start()

    barrier = pltpu.get_barrier_semaphore()

    def peers():
        ahead_first = (2 * me + 1) // nsp
        for i in range(nsp - 1):
            up = nsp - 1 - i - (i + me + 1) // nsp
            down = i + (nsp - 1 - me + i + 1) // nsp
            yield up * (1 - ahead_first) + down * ahead_first

    for peer in peers():
        pl.semaphore_signal(barrier, inc=1, device_id={"sp": peer}, device_id_type=MESH)
    for d in range(1, ntp):
        pl.semaphore_signal(barrier, inc=1, device_id={"tp": lax.rem(mine + d, ntp)}, device_id_type=MESH)

    zero = jnp.zeros((SUB, LANES), jnp.float32)
    blank = jnp.zeros((tiles, LANES), jnp.float32)

    def at(u, k, shift=0):
        return pl.ds(u * APART + k + shift, SUB, stride=PITCH)

    def spot(g, shift=0):
        return pl.ds(g // SUB * APART + g % SUB * PITCH + shift, SUB)

    def lanes(j):
        return pl.ds(j * LANES if isinstance(j, int) else pl.multiple_of(j * LANES, LANES), LANES)

    def keeps(g, members):
        for j in members:
            decay_s[j, spot(g), :] = jnp.exp2(decay_v[pl.ds(g * SUB, SUB), lanes(j)] * (-LOG2E / length))

    def pushes(g, members):
        for j in members:
            value = drive_v[pl.ds(g * SUB, 2 * SUB), lanes(j)].astype(jnp.float32)
            push_s[j, spot(g, PUSH), :] = value[:SUB]
            push_s[j, spot(g + 1, PUSH), :] = value[SUB:]

    def inside(block):
        return range(block[0] * SUB, (block[-1] + 1) * SUB, 2)

    def scan(block, members):
        spans = {}
        for k in range(SUB):
            for u in block:
                for n, j in enumerate(members):
                    keep = decay_s[j, at(u, k), :]
                    push = push_s[j, at(u, k, PUSH), :]
                    if k == 0:
                        spans[u, n] = keep, push, push
                    else:
                        prod, fwd, bwd = spans[u, n]
                        spans[u, n] = prod * keep, keep * fwd + push, bwd + prod * push
        for (u, n), span in spans.items():
            for q in range(3):
                ends_s[q, u, pl.ds(members[n] * near, SUB), :] = span[q]

    def chunk(u, i):
        return tuple(ends_s[q, u, pl.ds(i, tiles, stride=near), :] for q in range(3))

    whole = None
    for n, block in enumerate(blocks):
        if n == final:
            pltpu.make_async_copy(gate, gate_v, local.at[0]).start()
            pltpu.make_async_copy(gain, gain_v, local.at[1]).start()
            drain(decay_v.at[band(block)], local.at[n])
        else:
            drain(fwd_s.at[:, pl.ds(0, len(block) * UNIT * 3 // 2)], local.at[n])
        wide = max(1, min(tiles, SUB // len(block)))
        parts = [range(m, m + wide) for m in range(0, tiles, wide)]
        for members in parts:
            for g in inside(block):
                keeps(g, members)
                keeps(g + 1, members)
                if n < final:
                    pushes(g, members)
            if n < final:
                scan(block, members)
        if n == final:
            drain(drive_v.at[band(block)], local.at[n + 1])
            for members in parts:
                for g in inside(block):
                    pushes(g, members)
                scan(block, members)
        for u in block:
            unit = reduced([chunk(u, i) for i in range(SUB)])
            whole = unit if whole is None else joined(whole, unit)

    totals[me, 1], totals[me, 2], totals[me, 0] = whole

    pl.semaphore_wait(barrier, nsp + ntp - 2)

    def share(peer, d):
        part = pl.ds(1 - (me + d) // nsp, 2)
        return pltpu.make_async_remote_copy(
            src_ref=totals.at[me, part],
            dst_ref=totals.at[me, part],
            send_sem=local.at[2],
            recv_sem=trecv.at[d - 1],
            device_id={"sp": peer},
            device_id_type=MESH,
        )

    sends = [share(peer, lax.rem(peer - me + nsp, nsp)) for peer in peers()]
    for copy in sends:
        copy.start()

    def rise(u, carry):
        prod, enter = carry
        for i in range(SUB):
            edge_s[0, u, pl.ds(i * near, tiles), :] = prod
            edge_s[1, u, pl.ds(i * near, tiles), :] = enter
            keep, fwd, _ = chunk(u, i)
            prod, enter = prod * keep, keep * enter + fwd
        return prod, enter

    def fall(n, carry):
        prod, enter = carry
        u = units - 1 - n
        for i in reversed(range(SUB)):
            edge_s[2, u, pl.ds(i * near, tiles), :] = prod
            edge_s[3, u, pl.ds(i * near, tiles), :] = enter
            keep, _, bwd = chunk(u, i)
            prod, enter = prod * keep, keep * enter + bwd
        return prod, enter

    lax.fori_loop(0, units, rise, (blank + 1.0, blank))
    lax.fori_loop(0, units, fall, (blank + 1.0, blank))

    drain(gate_v, local.at[0])

    def edges(q, j):
        return [edge_s[q, u, pl.ds(j, SUB, stride=near), :] for u in range(units)]

    def packed(u, k):
        return pl.ds((u * SUB + k) * SUB, SUB)

    def gates(j, carry):
        for g in range(0, groups, 2):
            value = gate_v[pl.ds(g * SUB, 2 * SUB), lanes(j)].astype(jnp.float32)
            value = 1.0 / (1.0 + jnp.exp2(value * -LOG2E))
            sig_s[j, spot(g, SIG), :] = value[:SUB]
            sig_s[j, spot(g + 1, SIG), :] = value[SUB:]
        pre, fwd = edges(0, j), edges(1, j)
        for k in range(SUB):
            for u in range(units):
                keep = decay_s[j, at(u, k), :]
                fwd[u] = keep * fwd[u] + push_s[j, at(u, k, PUSH), :]
                pre[u] = keep * pre[u]
                fwd_s[j, packed(u, k), :] = fwd[u]
                pre_s[j, packed(u, k), :] = pre[u]
        suf, bwd = edges(2, j), edges(3, j)
        for k in reversed(range(SUB)):
            for u in range(units):
                keep = decay_s[j, at(u, k), :]
                sig = sig_s[j, at(u, k, SIG), :]
                bwd[u] = keep * bwd[u] + push_s[j, at(u, k, PUSH), :]
                suf[u] = keep * suf[u]
                base_s[j, at(u, k), :] = (fwd_s[j, packed(u, k), :] + bwd[u]) * sig
                left_s[j, at(u, k, LEFT), :] = pre_s[j, packed(u, k), :] * sig
                right_s[j, at(u, k, RIGHT), :] = suf[u] * sig
        return carry

    lax.fori_loop(0, tiles, gates, 0)

    def arrive(n, carry):
        share(me, carry - n).wait_recv()
        return carry

    def spread(q, j):
        return jnp.broadcast_to(enter_s[q, pl.ds(j, 1), :], (SUB, LANES))

    lax.fori_loop(0, me, arrive, me)

    def join(s, enter):
        return totals[s, 1] * enter + totals[s, 2]

    enter_s[0] = lax.fori_loop(0, me, join, blank)

    def settle(j, carry):
        enter = spread(0, j)
        for g in range(groups):
            base_s[j, spot(g), :] = base_s[j, spot(g), :] + left_s[j, spot(g, LEFT), :] * enter
        return carry

    lax.fori_loop(0, tiles, settle, 0)

    lax.fori_loop(0, nsp - 2 - me, arrive, nsp - 1)

    def prepend(n, carry):
        enter, span = carry
        e = me + 1 + n
        return enter + span * totals[e, 0], span * totals[e, 1]

    enter, span = lax.fori_loop(0, nsp - 2 - me, prepend, (blank, blank + 1.0))
    enter_s[1] = enter
    enter_s[2] = jnp.where(me < nsp - 1, span, 0.0)
    enters = [(spread(1, j), spread(2, j)) for j in range(tiles)]

    @pl.when(me < nsp - 1)
    def _():
        share(me, me + 1).wait_recv()

    enters = [
        enter + span * jnp.broadcast_to(totals[nsp - 1, 0, pl.ds(j, 1), :], (SUB, LANES))
        for j, (enter, span) in enumerate(enters)
    ]
    width = powers.shape[-1]
    lane = lax.broadcasted_iota(jnp.int32, (SUB, width), 1)
    sums = jnp.zeros((SUB, width), jnp.float32)
    for g in range(groups):
        squares = zero
        for j in range(tiles):
            value = base_s[j, spot(g), :] + right_s[j, spot(g, RIGHT), :] * enters[j]
            squares = squares + value * value
        sums = jnp.where(lane == g, jnp.sum(squares, axis=1, keepdims=True), sums)
    powers[mine] = sums

    tells = []
    for d in sorted(range(1, ntp), key=lambda d: abs(2 * d - ntp)):
        tells.append(pltpu.make_async_remote_copy(
            src_ref=powers.at[mine],
            dst_ref=powers.at[mine],
            send_sem=local.at[3],
            recv_sem=precv,
            device_id={"tp": lax.rem(mine + d, ntp)},
            device_id_type=MESH,
        ))
    for copy in tells:
        copy.start()
    enter_s[1] = enter_s[1] + enter_s[2] * totals[nsp - 1, 0]
    drain(gain_v, local.at[1])

    def weigh(j, carry):
        own = jnp.broadcast_to(gain_v[pl.ds(j, 1), :], (SUB, LANES))
        enter = spread(1, j)
        for g in range(groups):
            value = base_s[j, spot(g), :] + right_s[j, spot(g, RIGHT), :] * enter
            gated[j, pl.ds(g * SUB, SUB), :] = value * own
        return carry

    lax.fori_loop(0, tiles, weigh, 0)

    drain(totals.at[pl.ds(0, nsp - 1), pl.ds(0, 2)], local.at[2])
    drain(powers.at[pl.ds(0, ntp - 1)], local.at[3])
    drain(powers.at[pl.ds(0, ntp - 1)], precv)

    power = powers[0]
    for s in range(1, ntp):
        power = power + powers[s]
    power = power * (1.0 / (length * channels * ntp))
    inverse[...] = lax.rsqrt(power + 1e-06) * length ** (-0.5)


def emit(gated, inverse, out, staged, sem):
    rows, channels = out.shape
    tiles = channels // LANES
    pair = 2 * SUB
    block = rows // SUB
    scale = inverse[...]
    for b in range(SUB):
        for row in range(b * block, (b + 1) * block, pair):
            g = row // SUB
            own = jnp.concatenate([
                jnp.broadcast_to(scale[:, g + n : g + n + 1], (SUB, LANES)) for n in range(2)
            ], axis=0)
            for j in range(tiles):
                staged[pl.ds(row, pair), pl.ds(j * LANES, LANES)] = (
                    gated[j, pl.ds(row, pair), :] * own
                ).astype(jnp.bfloat16)
        dense = pl.ds(b * block, block)
        pltpu.make_async_copy(staged.at[dense], out.at[dense], sem).start()
    pltpu.make_async_copy(staged, out, sem).wait()


def body(nsp, ntp, decay_rate, drive_in, gate_in, norm_gain):
    batch, rows, channels = decay_rate.shape
    tiles = channels // LANES
    units = rows // UNIT
    near = spaced(max(SUB, tiles))
    width = -(-(rows // SUB) // LANES) * LANES
    plane = pltpu.VMEM((tiles, rows, LANES), jnp.float32)
    wide = pltpu.VMEM((tiles, -(-(units * APART) // SUB) * SUB + SUB, LANES), jnp.float32)
    half = pltpu.VMEM((rows, channels), jnp.bfloat16)
    outside = pl.BlockSpec(memory_space=pltpu.HBM)
    vmem = pl.BlockSpec(memory_space=pltpu.VMEM)
    gated, inverse = pl.pallas_call(
        functools.partial(kernel, nsp, ntp),
        out_shape=(
            pltpu.VMEM((tiles, rows, LANES), jnp.float32),
            pltpu.VMEM((SUB, width), jnp.float32),
        ),
        in_specs=[outside] * 4,
        out_specs=(vmem, vmem),
        scratch_shapes=[
            pltpu.VMEM((rows, channels), jnp.float32), half, half,
            wide, wide, wide, plane, plane, wide, wide, wide,
            pltpu.VMEM((3, units, tiles * near, LANES), jnp.float32),
            pltpu.VMEM((4, units, SUB * near, LANES), jnp.float32),
            pltpu.VMEM((3, tiles, LANES), jnp.float32),
            pltpu.VMEM((nsp, 3, tiles, LANES), jnp.float32),
            pltpu.VMEM((ntp, SUB, width), jnp.float32),
            pltpu.VMEM((tiles, LANES), jnp.float32),
            pltpu.SemaphoreType.DMA((len(blocked(units)) + 1,)),
            pltpu.SemaphoreType.DMA((nsp - 1,)),
            pltpu.SemaphoreType.DMA,
        ],
        compiler_params=pltpu.CompilerParams(
            collective_id=0, has_side_effects=True, vmem_limit_bytes=52 * 1024 * 1024
        ),
    )(*(
        pltpu.with_memory_space_constraint(value, pltpu.HBM)
        for value in (
            decay_rate.reshape(rows, channels),
            drive_in.reshape(rows, channels),
            gate_in.reshape(rows, channels),
            norm_gain.reshape(tiles, LANES),
        )
    ))
    result = pl.pallas_call(
        emit,
        out_shape=jax.ShapeDtypeStruct((rows, channels), jnp.bfloat16),
        in_specs=[vmem, vmem],
        out_specs=outside,
        scratch_shapes=[
            pltpu.VMEM((rows, channels), jnp.bfloat16),
            pltpu.SemaphoreType.DMA,
        ],
        compiler_params=pltpu.CompilerParams(vmem_limit_bytes=32 * 1024 * 1024),
    )(
        pltpu.with_memory_space_constraint(gated, pltpu.VMEM),
        pltpu.with_memory_space_constraint(inverse, pltpu.VMEM),
    )
    return result.reshape(batch, rows, channels)


def solution(mesh):
    in_specs = (P(None, "sp", "tp"), P(None, "sp", "tp"), P(None, "sp", "tp"), P("tp"))
    out_specs = P(None, "sp", "tp")
    local = functools.partial(body, mesh.shape["sp"], mesh.shape["tp"])
    return jax.shard_map(local, mesh=mesh, in_specs=in_specs, out_specs=out_specs, check_vma=False)
```

```python
import functools

import jax
import jax.numpy as jnp
from jax import lax
from jax.experimental import pallas as pl
from jax.experimental.pallas import tpu as pltpu
from jax.sharding import PartitionSpec as P

LANES = 128
SUB = 8
LOG2E = 1.4426950408889634
MESH = pl.DeviceIdType.MESH


def spaced(steps):
    return steps + next(more for more in range(4, 40, 4) if (steps + more) % 8 == 4)


PITCH = spaced(SUB)
UNIT = SUB * SUB
APART = SUB * PITCH + 1
PUSH, SIG, LEFT, RIGHT = 2, 1, 1, 8


def joined(early, late):
    (p, f, b), (q, g, c) = early, late
    return p * q, q * f + g, b + p * c


def reduced(spans):
    while len(spans) > 1:
        spans = [joined(*pair) for pair in zip(spans[::2], spans[1::2])] + spans[len(spans) - len(spans) % 2 :]
    return spans[0]


def blocked(units):
    return [range(u, u + 2) for u in range(0, units - 2, 2)] + [range(u, u + 1) for u in range(units - 2 + units % 2, units)]


def kernel(
    nsp, ntp, decay, drive, gate, gain, gated, inverse,
    decay_v, drive_v, gate_v, decay_s, push_s, sig_s, fwd_s, pre_s, base_s, left_s, right_s,
    ends_s, edge_s, enter_s, totals, powers, gain_v, local, trecv, precv,
):
    rows, channels = decay.shape
    tiles = channels // LANES
    units = rows // UNIT
    groups = rows // SUB
    length = rows * nsp
    near = spaced(max(SUB, tiles))
    me, mine = lax.axis_index("sp"), lax.axis_index("tp")
    blocks = blocked(units)
    final = len(blocks) - 1

    def band(block):
        return pl.ds(block[0] * UNIT, len(block) * UNIT)

    def drain(ref, sem):
        pltpu.make_async_copy(ref, ref, sem).wait()

    for n, block in enumerate(blocks):
        pltpu.make_async_copy(decay.at[band(block)], decay_v.at[band(block)], local.at[n]).start()
        pltpu.make_async_copy(
            drive.at[band(block)], drive_v.at[band(block)], local.at[n if n < final else n + 1]
        ).start()

    barrier = pltpu.get_barrier_semaphore()

    def peers():
        ahead_first = (2 * me + 1) // nsp
        for i in range(nsp - 1):
            up = nsp - 1 - i - (i + me + 1) // nsp
            down = i + (nsp - 1 - me + i + 1) // nsp
            yield up * (1 - ahead_first) + down * ahead_first

    for peer in peers():
        pl.semaphore_signal(barrier, inc=1, device_id={"sp": peer}, device_id_type=MESH)
    for d in range(1, ntp):
        pl.semaphore_signal(barrier, inc=1, device_id={"tp": lax.rem(mine + d, ntp)}, device_id_type=MESH)

    zero = jnp.zeros((SUB, LANES), jnp.float32)
    blank = jnp.zeros((tiles, LANES), jnp.float32)

    def at(u, k, shift=0):
        return pl.ds(u * APART + k + shift, SUB, stride=PITCH)

    def spot(g, shift=0):
        return pl.ds(g // SUB * APART + g % SUB * PITCH + shift, SUB)

    def lanes(j):
        return pl.ds(j * LANES if isinstance(j, int) else pl.multiple_of(j * LANES, LANES), LANES)

    def keeps(g, members):
        for j in members:
            decay_s[j, spot(g), :] = jnp.exp2(decay_v[pl.ds(g * SUB, SUB), lanes(j)] * (-LOG2E / length))

    def pushes(g, members):
        for j in members:
            value = drive_v[pl.ds(g * SUB, 2 * SUB), lanes(j)].astype(jnp.float32)
            push_s[j, spot(g, PUSH), :] = value[:SUB]
            push_s[j, spot(g + 1, PUSH), :] = value[SUB:]

    def inside(block):
        return range(block[0] * SUB, (block[-1] + 1) * SUB, 2)

    def scan(block, members):
        spans = {}
        for k in range(SUB):
            for u in block:
                for n, j in enumerate(members):
                    keep = decay_s[j, at(u, k), :]
                    push = push_s[j, at(u, k, PUSH), :]
                    if k == 0:
                        spans[u, n] = keep, push, push
                    else:
                        prod, fwd, bwd = spans[u, n]
                        spans[u, n] = prod * keep, keep * fwd + push, bwd + prod * push
        for (u, n), span in spans.items():
            for q in range(3):
                ends_s[q, u, pl.ds(members[n] * near, SUB), :] = span[q]

    def chunk(u, i):
        return tuple(ends_s[q, u, pl.ds(i, tiles, stride=near), :] for q in range(3))

    whole = []

    def settled(block):
        for u in block:
            whole.append(reduced([chunk(u, i) for i in range(SUB)]))
        whole[:] = [reduced(whole)]

    for n, block in enumerate(blocks):
        if n == final:
            pltpu.make_async_copy(gate, gate_v, local.at[0]).start()
            pltpu.make_async_copy(gain, gain_v, local.at[1]).start()
            drain(decay_v.at[band(block)], local.at[n])
        else:
            drain(fwd_s.at[:, pl.ds(0, len(block) * UNIT * 3 // 2)], local.at[n])
        wide = max(1, min(tiles, SUB // len(block)))
        parts = [range(m, m + wide) for m in range(0, tiles, wide)]
        for members in parts:
            for g in inside(block):
                keeps(g, members)
                keeps(g + 1, members)
                if n < final:
                    pushes(g, members)
            if n > 0 and members is parts[0]:
                settled(blocks[n - 1])
            if n < final:
                scan(block, members)
        if n == final:
            drain(drive_v.at[band(block)], local.at[n + 1])
            for members in parts:
                for g in inside(block):
                    pushes(g, members)
                scan(block, members)
    settled(blocks[final])

    totals[me, 1], totals[me, 2], totals[me, 0] = whole[0]

    pl.semaphore_wait(barrier, nsp + ntp - 2)

    def share(peer, row, kind, sem):
        return pltpu.make_async_remote_copy(
            src_ref=totals.at[me, row],
            dst_ref=totals.at[me, row],
            send_sem=local.at[sem],
            recv_sem=trecv.at[kind],
            device_id={"sp": peer},
            device_id_type=MESH,
        )

    inner = jnp.logical_and(me > 0, me < nsp - 1)
    ways = []
    for peer in peers():
        above = (peer + nsp - me) // nsp
        ways.append((peer, 2 * above, (1 - above) * (1 + me // (nsp - 1))))
    for peer, row, kind in ways:
        share(peer, row, kind, 2).start()

    @pl.when(inner)
    def _():
        for peer, _, kind in ways:
            share(peer, 1, kind, 4).start()

    def counted(count, sem):
        for v in range(nsp):
            if count(v) > 0:

                @pl.when(me == v)
                def _(n=count(v)):
                    drain(fwd_s.at[0, pl.ds(0, n * tiles)], sem)

    def rise(u, carry):
        prod, enter = carry
        for i in range(SUB):
            edge_s[0, u, pl.ds(i * near, tiles), :] = prod
            edge_s[1, u, pl.ds(i * near, tiles), :] = enter
            keep, fwd, _ = chunk(u, i)
            prod, enter = prod * keep, keep * enter + fwd
        return prod, enter

    def fall(n, carry):
        prod, enter = carry
        u = units - 1 - n
        for i in reversed(range(SUB)):
            edge_s[2, u, pl.ds(i * near, tiles), :] = prod
            edge_s[3, u, pl.ds(i * near, tiles), :] = enter
            keep, _, bwd = chunk(u, i)
            prod, enter = prod * keep, keep * enter + bwd
        return prod, enter

    lax.fori_loop(0, units, rise, (blank + 1.0, blank))
    lax.fori_loop(0, units, fall, (blank + 1.0, blank))

    drain(gate_v, local.at[0])

    def edges(q, j):
        return [edge_s[q, u, pl.ds(j, SUB, stride=near), :] for u in range(units)]

    def packed(u, k):
        return pl.ds((u * SUB + k) * SUB, SUB)

    def gates(j, carry):
        for g in range(0, groups, 2):
            value = gate_v[pl.ds(g * SUB, 2 * SUB), lanes(j)].astype(jnp.float32)
            value = 1.0 / (1.0 + jnp.exp2(value * -LOG2E))
            sig_s[j, spot(g, SIG), :] = value[:SUB]
            sig_s[j, spot(g + 1, SIG), :] = value[SUB:]
        pre, fwd = edges(0, j), edges(1, j)
        for k in range(SUB):
            for u in range(units):
                keep = decay_s[j, at(u, k), :]
                fwd[u] = keep * fwd[u] + push_s[j, at(u, k, PUSH), :]
                pre[u] = keep * pre[u]
                fwd_s[j, packed(u, k), :] = fwd[u]
                pre_s[j, packed(u, k), :] = pre[u]
        suf, bwd = edges(2, j), edges(3, j)
        for k in reversed(range(SUB)):
            for u in range(units):
                keep = decay_s[j, at(u, k), :]
                sig = sig_s[j, at(u, k, SIG), :]
                bwd[u] = keep * bwd[u] + push_s[j, at(u, k, PUSH), :]
                suf[u] = keep * suf[u]
                base_s[j, at(u, k), :] = (fwd_s[j, packed(u, k), :] + bwd[u]) * sig
                left_s[j, at(u, k, LEFT), :] = pre_s[j, packed(u, k), :] * sig
                right_s[j, at(u, k, RIGHT), :] = suf[u] * sig
        return carry

    lax.fori_loop(0, tiles, gates, 0)

    def spread(q, j):
        return jnp.broadcast_to(enter_s[q, pl.ds(j, 1), :], (SUB, LANES))

    counted(lambda v: v + max(v - 1, 0), trecv.at[0])

    def join(s, enter):
        return totals[s, 1] * enter + totals[s, 2]

    enter_s[0] = lax.fori_loop(1, me, join, jnp.where(me > 0, totals[0, 2], 0.0))

    def settle(j, carry):
        enter = spread(0, j)
        for g in range(groups):
            base_s[j, spot(g), :] = base_s[j, spot(g), :] + left_s[j, spot(g, LEFT), :] * enter
        return carry

    lax.fori_loop(0, tiles, settle, 0)

    counted(lambda v: 2 * (nsp - 2 - v), trecv.at[1])

    def prepend(n, carry):
        enter, span = carry
        e = me + 1 + n
        return enter + span * totals[e, 0], span * totals[e, 1]

    enter, span = lax.fori_loop(0, nsp - 2 - me, prepend, (blank, blank + 1.0))
    enter_s[1] = enter
    enter_s[2] = jnp.where(me < nsp - 1, span, 0.0)
    enters = [(spread(1, j), spread(2, j)) for j in range(tiles)]

    @pl.when(me < nsp - 1)
    def _():
        drain(totals.at[0, 0], trecv.at[2])

    enters = [
        enter + span * jnp.broadcast_to(totals[nsp - 1, 0, pl.ds(j, 1), :], (SUB, LANES))
        for j, (enter, span) in enumerate(enters)
    ]
    width = powers.shape[-1]
    lane = lax.broadcasted_iota(jnp.int32, (SUB, width), 1)
    sums = jnp.zeros((SUB, width), jnp.float32)
    for g in range(groups):
        squares = zero
        for j in range(tiles):
            value = base_s[j, spot(g), :] + right_s[j, spot(g, RIGHT), :] * enters[j]
            squares = squares + value * value
        sums = jnp.where(lane == g, jnp.sum(squares, axis=1, keepdims=True), sums)
    powers[mine] = sums

    tells = []
    for d in sorted(range(1, ntp), key=lambda d: abs(2 * d - ntp)):
        tells.append(pltpu.make_async_remote_copy(
            src_ref=powers.at[mine],
            dst_ref=powers.at[mine],
            send_sem=local.at[3],
            recv_sem=precv,
            device_id={"tp": lax.rem(mine + d, ntp)},
            device_id_type=MESH,
        ))
    for copy in tells:
        copy.start()
    enter_s[1] = enter_s[1] + enter_s[2] * totals[nsp - 1, 0]
    drain(gain_v, local.at[1])

    def weigh(j, carry):
        own = jnp.broadcast_to(gain_v[pl.ds(j, 1), :], (SUB, LANES))
        enter = spread(1, j)
        for g in range(groups):
            value = base_s[j, spot(g), :] + right_s[j, spot(g, RIGHT), :] * enter
            gated[j, pl.ds(g * SUB, SUB), :] = value * own
        return carry

    lax.fori_loop(0, tiles, weigh, 0)

    drain(fwd_s.at[0, pl.ds(0, (nsp - 1) * tiles)], local.at[2])

    @pl.when(inner)
    def _():
        drain(fwd_s.at[0, pl.ds(0, (nsp - 1) * tiles)], local.at[4])

    drain(powers.at[pl.ds(0, ntp - 1)], local.at[3])
    drain(powers.at[pl.ds(0, ntp - 1)], precv)

    power = powers[0]
    for s in range(1, ntp):
        power = power + powers[s]
    power = power * (1.0 / (length * channels * ntp))
    inverse[...] = lax.rsqrt(power + 1e-06) * length ** (-0.5)


def emit(gated, inverse, out, staged, sem):
    rows, channels = out.shape
    tiles = channels // LANES
    pair = 2 * SUB
    parts = rows // (2 * pair)
    block = rows // parts
    scale = inverse[...]
    for b in range(parts):
        for row in range(b * block, (b + 1) * block, pair):
            g = row // SUB
            own = jnp.concatenate([
                jnp.broadcast_to(scale[:, g + n : g + n + 1], (SUB, LANES)) for n in range(2)
            ], axis=0)
            for j in range(tiles):
                staged[pl.ds(row, pair), pl.ds(j * LANES, LANES)] = (
                    gated[j, pl.ds(row, pair), :] * own
                ).astype(jnp.bfloat16)
        dense = pl.ds(b * block, block)
        pltpu.make_async_copy(staged.at[dense], out.at[dense], sem).start()
    pltpu.make_async_copy(staged, out, sem).wait()


def body(nsp, ntp, decay_rate, drive_in, gate_in, norm_gain):
    batch, rows, channels = decay_rate.shape
    tiles = channels // LANES
    units = rows // UNIT
    near = spaced(max(SUB, tiles))
    width = -(-(rows // SUB) // LANES) * LANES
    plane = pltpu.VMEM((tiles, rows, LANES), jnp.float32)
    wide = pltpu.VMEM((tiles, -(-(units * APART) // SUB) * SUB + SUB, LANES), jnp.float32)
    half = pltpu.VMEM((rows, channels), jnp.bfloat16)
    outside = pl.BlockSpec(memory_space=pltpu.HBM)
    vmem = pl.BlockSpec(memory_space=pltpu.VMEM)
    gated, inverse = pl.pallas_call(
        functools.partial(kernel, nsp, ntp),
        out_shape=(
            pltpu.VMEM((tiles, rows, LANES), jnp.float32),
            pltpu.VMEM((SUB, width), jnp.float32),
        ),
        in_specs=[outside] * 4,
        out_specs=(vmem, vmem),
        scratch_shapes=[
            pltpu.VMEM((rows, channels), jnp.float32), half, half,
            wide, wide, wide, plane, plane, wide, wide, wide,
            pltpu.VMEM((3, units, tiles * near, LANES), jnp.float32),
            pltpu.VMEM((4, units, SUB * near, LANES), jnp.float32),
            pltpu.VMEM((3, tiles, LANES), jnp.float32),
            pltpu.VMEM((nsp, 3, tiles, LANES), jnp.float32),
            pltpu.VMEM((ntp, SUB, width), jnp.float32),
            pltpu.VMEM((tiles, LANES), jnp.float32),
            pltpu.SemaphoreType.DMA((len(blocked(units)) + 1,)),
            pltpu.SemaphoreType.DMA((3,)),
            pltpu.SemaphoreType.DMA,
        ],
        compiler_params=pltpu.CompilerParams(
            collective_id=0, has_side_effects=True, vmem_limit_bytes=52 * 1024 * 1024
        ),
    )(*(
        pltpu.with_memory_space_constraint(value, pltpu.HBM)
        for value in (
            decay_rate.reshape(rows, channels),
            drive_in.reshape(rows, channels),
            gate_in.reshape(rows, channels),
            norm_gain.reshape(tiles, LANES),
        )
    ))
    result = pl.pallas_call(
        emit,
        out_shape=jax.ShapeDtypeStruct((rows, channels), jnp.bfloat16),
        in_specs=[vmem, vmem],
        out_specs=outside,
        scratch_shapes=[
            pltpu.VMEM((rows, channels), jnp.bfloat16),
            pltpu.SemaphoreType.DMA,
        ],
        compiler_params=pltpu.CompilerParams(vmem_limit_bytes=32 * 1024 * 1024),
    )(
        pltpu.with_memory_space_constraint(gated, pltpu.VMEM),
        pltpu.with_memory_space_constraint(inverse, pltpu.VMEM),
    )
    return result.reshape(batch, rows, channels)


def solution(mesh):
    in_specs = (P(None, "sp", "tp"), P(None, "sp", "tp"), P(None, "sp", "tp"), P("tp"))
    out_specs = P(None, "sp", "tp")
    local = functools.partial(body, mesh.shape["sp"], mesh.shape["tp"])
    return jax.shard_map(local, mesh=mesh, in_specs=in_specs, out_specs=out_specs, check_vma=False)
```

```python
import functools

import jax
import jax.numpy as jnp
from jax import lax
from jax.experimental import pallas as pl
from jax.experimental.pallas import tpu as pltpu
from jax.sharding import PartitionSpec as P

LANES = 128
SUB = 8
LOG2E = 1.4426950408889634
MESH = pl.DeviceIdType.MESH


def spaced(steps):
    return steps + next(more for more in range(4, 40, 4) if (steps + more) % 8 == 4)


PITCH = spaced(SUB)
UNIT = SUB * SUB
APART = SUB * PITCH + 1
PUSH, SIG, LEFT, RIGHT = 2, 1, 1, 8


def joined(early, late):
    (p, f, b), (q, g, c) = early, late
    return p * q, q * f + g, b + p * c


def reduced(spans):
    while len(spans) > 1:
        spans = [joined(*pair) for pair in zip(spans[::2], spans[1::2])] + spans[len(spans) - len(spans) % 2 :]
    return spans[0]


def blocked(units):
    return [range(u, u + 2) for u in range(0, units - 2, 2)] + [range(u, u + 1) for u in range(units - 2 + units % 2, units)]


def kernel(
    nsp, ntp, decay, drive, gate, gain, gated, inverse,
    decay_v, drive_v, gate_v, decay_s, push_s, sig_s, fwd_s, pre_s, base_s, left_s, right_s,
    ends_s, edge_s, enter_s, totals, powers, gain_v, local, trecv, precv,
):
    rows, channels = decay.shape
    tiles = channels // LANES
    units = rows // UNIT
    groups = rows // SUB
    length = rows * nsp
    near = spaced(max(SUB, tiles))
    me, mine = lax.axis_index("sp"), lax.axis_index("tp")
    blocks = blocked(units)
    final = len(blocks) - 1

    def band(block):
        return pl.ds(block[0] * UNIT, len(block) * UNIT)

    def drain(ref, sem):
        pltpu.make_async_copy(ref, ref, sem).wait()

    for n, block in enumerate(blocks):
        pltpu.make_async_copy(decay.at[band(block)], decay_v.at[band(block)], local.at[n]).start()
        pltpu.make_async_copy(
            drive.at[band(block)], drive_v.at[band(block)], local.at[n if n < final else n + 1]
        ).start()

    barrier = pltpu.get_barrier_semaphore()

    def peers():
        ahead_first = (2 * me + 1) // nsp
        for i in range(nsp - 1):
            up = nsp - 1 - i - (i + me + 1) // nsp
            down = i + (nsp - 1 - me + i + 1) // nsp
            yield up * (1 - ahead_first) + down * ahead_first

    for peer in peers():
        pl.semaphore_signal(barrier, inc=1, device_id={"sp": peer}, device_id_type=MESH)
    for d in range(1, ntp):
        pl.semaphore_signal(barrier, inc=1, device_id={"tp": lax.rem(mine + d, ntp)}, device_id_type=MESH)

    zero = jnp.zeros((SUB, LANES), jnp.float32)
    blank = jnp.zeros((tiles, LANES), jnp.float32)

    def at(u, k, shift=0):
        return pl.ds(u * APART + k + shift, SUB, stride=PITCH)

    def spot(g, shift=0):
        return pl.ds(g // SUB * APART + g % SUB * PITCH + shift, SUB)

    def lanes(j):
        return pl.ds(j * LANES if isinstance(j, int) else pl.multiple_of(j * LANES, LANES), LANES)

    def keeps(g, members):
        for j in members:
            decay_s[j, spot(g), :] = jnp.exp2(decay_v[pl.ds(g * SUB, SUB), lanes(j)] * (-LOG2E / length))

    def pushes(g, members):
        for j in members:
            value = drive_v[pl.ds(g * SUB, 2 * SUB), lanes(j)].astype(jnp.float32)
            push_s[j, spot(g, PUSH), :] = value[:SUB]
            push_s[j, spot(g + 1, PUSH), :] = value[SUB:]

    def inside(block):
        return range(block[0] * SUB, (block[-1] + 1) * SUB, 2)

    def scan(block, members):
        spans = {}
        for k in range(SUB):
            for u in block:
                for n, j in enumerate(members):
                    keep = decay_s[j, at(u, k), :]
                    push = push_s[j, at(u, k, PUSH), :]
                    if k == 0:
                        spans[u, n] = keep, push, push
                    else:
                        prod, fwd, bwd = spans[u, n]
                        spans[u, n] = prod * keep, keep * fwd + push, bwd + prod * push
        for (u, n), span in spans.items():
            for q in range(3):
                ends_s[q, u, pl.ds(members[n] * near, SUB), :] = span[q]

    def chunk(u, i):
        return tuple(ends_s[q, u, pl.ds(i, tiles, stride=near), :] for q in range(3))

    whole = []

    def settled(block):
        for u in block:
            whole.append(reduced([chunk(u, i) for i in range(SUB)]))
        whole[:] = [reduced(whole)]

    for n, block in enumerate(blocks):
        if n == final:
            pltpu.make_async_copy(gate, gate_v, local.at[0]).start()
            pltpu.make_async_copy(gain, gain_v, local.at[1]).start()
            drain(decay_v.at[band(block)], local.at[n])
        else:
            drain(fwd_s.at[:, pl.ds(0, len(block) * UNIT * 3 // 2)], local.at[n])
        wide = max(1, min(tiles, SUB // len(block)))
        parts = [range(m, m + wide) for m in range(0, tiles, wide)]
        for members in parts:
            for g in inside(block):
                keeps(g, members)
                keeps(g + 1, members)
                if n < final:
                    pushes(g, members)
            if n > 0 and members is parts[0]:
                settled(blocks[n - 1])
            if n < final:
                scan(block, members)
        if n == final:
            pl.semaphore_wait(barrier, nsp + ntp - 2)
            drain(drive_v.at[band(block)], local.at[n + 1])
            for members in parts:
                for g in inside(block):
                    pushes(g, members)
                scan(block, members)
    settled(blocks[final])

    totals[me, 1], totals[me, 2], totals[me, 0] = whole[0]


    def share(peer, row, kind, sem):
        return pltpu.make_async_remote_copy(
            src_ref=totals.at[me, row],
            dst_ref=totals.at[me, row],
            send_sem=local.at[sem],
            recv_sem=trecv.at[kind],
            device_id={"sp": peer},
            device_id_type=MESH,
        )

    inner = jnp.logical_and(me > 0, me < nsp - 1)
    ways = []
    for peer in peers():
        above = (peer + nsp - me) // nsp
        ways.append((peer, 2 * above, (1 - above) * (1 + me // (nsp - 1))))
    for peer, row, kind in ways:
        share(peer, row, kind, 2).start()

    @pl.when(inner)
    def _():
        for peer, _, kind in ways:
            share(peer, 1, kind, 4).start()

    def counted(count, sem):
        for v in range(nsp):
            if count(v) > 0:

                @pl.when(me == v)
                def _(n=count(v)):
                    drain(fwd_s.at[0, pl.ds(0, n * tiles)], sem)

    def rise(u, carry):
        prod, enter = carry
        for i in range(SUB):
            edge_s[0, u, pl.ds(i * near, tiles), :] = prod
            edge_s[1, u, pl.ds(i * near, tiles), :] = enter
            keep, fwd, _ = chunk(u, i)
            prod, enter = prod * keep, keep * enter + fwd
        return prod, enter

    def fall(n, carry):
        prod, enter = carry
        u = units - 1 - n
        for i in reversed(range(SUB)):
            edge_s[2, u, pl.ds(i * near, tiles), :] = prod
            edge_s[3, u, pl.ds(i * near, tiles), :] = enter
            keep, _, bwd = chunk(u, i)
            prod, enter = prod * keep, keep * enter + bwd
        return prod, enter

    lax.fori_loop(0, units, rise, (blank + 1.0, blank))
    lax.fori_loop(0, units, fall, (blank + 1.0, blank))

    drain(gate_v, local.at[0])

    def edges(q, j):
        return [edge_s[q, u, pl.ds(j, SUB, stride=near), :] for u in range(units)]

    def packed(u, k):
        return pl.ds((u * SUB + k) * SUB, SUB)

    def gates(j, carry):
        for g in range(0, groups, 2):
            value = gate_v[pl.ds(g * SUB, 2 * SUB), lanes(j)].astype(jnp.float32)
            value = 1.0 / (1.0 + jnp.exp2(value * -LOG2E))
            sig_s[j, spot(g, SIG), :] = value[:SUB]
            sig_s[j, spot(g + 1, SIG), :] = value[SUB:]
        pre, fwd = edges(0, j), edges(1, j)
        for k in range(SUB):
            for u in range(units):
                keep = decay_s[j, at(u, k), :]
                fwd[u] = keep * fwd[u] + push_s[j, at(u, k, PUSH), :]
                pre[u] = keep * pre[u]
                fwd_s[j, packed(u, k), :] = fwd[u]
                pre_s[j, packed(u, k), :] = pre[u]
        suf, bwd = edges(2, j), edges(3, j)
        for k in reversed(range(SUB)):
            for u in range(units):
                keep = decay_s[j, at(u, k), :]
                sig = sig_s[j, at(u, k, SIG), :]
                bwd[u] = keep * bwd[u] + push_s[j, at(u, k, PUSH), :]
                suf[u] = keep * suf[u]
                base_s[j, at(u, k), :] = (fwd_s[j, packed(u, k), :] + bwd[u]) * sig
                left_s[j, at(u, k, LEFT), :] = pre_s[j, packed(u, k), :] * sig
                right_s[j, at(u, k, RIGHT), :] = suf[u] * sig
        return carry

    lax.fori_loop(0, tiles, gates, 0)

    def spread(q, j):
        return jnp.broadcast_to(enter_s[q, pl.ds(j, 1), :], (SUB, LANES))

    counted(lambda v: v + max(v - 1, 0), trecv.at[0])

    def join(s, enter):
        return totals[s, 1] * enter + totals[s, 2]

    enter_s[0] = lax.fori_loop(1, me, join, jnp.where(me > 0, totals[0, 2], 0.0))

    def settle(j, carry):
        enter = spread(0, j)
        for g in range(groups):
            base_s[j, spot(g), :] = base_s[j, spot(g), :] + left_s[j, spot(g, LEFT), :] * enter
        return carry

    lax.fori_loop(0, tiles, settle, 0)

    counted(lambda v: 2 * (nsp - 2 - v), trecv.at[1])

    def prepend(n, carry):
        enter, span = carry
        e = me + 1 + n
        return enter + span * totals[e, 0], span * totals[e, 1]

    enter, span = lax.fori_loop(0, nsp - 2 - me, prepend, (blank, blank + 1.0))
    enter_s[1] = enter
    enter_s[2] = jnp.where(me < nsp - 1, span, 0.0)
    enters = [(spread(1, j), spread(2, j)) for j in range(tiles)]

    @pl.when(me < nsp - 1)
    def _():
        drain(totals.at[0, 0], trecv.at[2])

    enters = [
        enter + span * jnp.broadcast_to(totals[nsp - 1, 0, pl.ds(j, 1), :], (SUB, LANES))
        for j, (enter, span) in enumerate(enters)
    ]
    width = powers.shape[-1]
    lane = lax.broadcasted_iota(jnp.int32, (SUB, width), 1)
    sums = jnp.zeros((SUB, width), jnp.float32)
    for g in range(groups):
        squares = zero
        for j in range(tiles):
            value = base_s[j, spot(g), :] + right_s[j, spot(g, RIGHT), :] * enters[j]
            squares = squares + value * value
        sums = jnp.where(lane == g, jnp.sum(squares, axis=1, keepdims=True), sums)
    powers[mine] = sums

    tells = []
    for d in sorted(range(1, ntp), key=lambda d: abs(2 * d - ntp)):
        tells.append(pltpu.make_async_remote_copy(
            src_ref=powers.at[mine],
            dst_ref=powers.at[mine],
            send_sem=local.at[3],
            recv_sem=precv,
            device_id={"tp": lax.rem(mine + d, ntp)},
            device_id_type=MESH,
        ))
    for copy in tells:
        copy.start()
    enter_s[1] = enter_s[1] + enter_s[2] * totals[nsp - 1, 0]
    drain(gain_v, local.at[1])

    def weigh(j, carry):
        own = jnp.broadcast_to(gain_v[pl.ds(j, 1), :], (SUB, LANES))
        enter = spread(1, j)
        for g in range(groups):
            value = base_s[j, spot(g), :] + right_s[j, spot(g, RIGHT), :] * enter
            gated[j, pl.ds(g * SUB, SUB), :] = value * own
        return carry

    lax.fori_loop(0, tiles, weigh, 0)

    drain(fwd_s.at[0, pl.ds(0, (nsp - 1) * tiles)], local.at[2])

    @pl.when(inner)
    def _():
        drain(fwd_s.at[0, pl.ds(0, (nsp - 1) * tiles)], local.at[4])

    drain(powers.at[pl.ds(0, ntp - 1)], local.at[3])
    drain(powers.at[pl.ds(0, ntp - 1)], precv)

    power = powers[0]
    for s in range(1, ntp):
        power = power + powers[s]
    power = power * (1.0 / (length * channels * ntp))
    inverse[...] = lax.rsqrt(power + 1e-06) * length ** (-0.5)


def emit(gated, inverse, out, staged, sem):
    rows, channels = out.shape
    tiles = channels // LANES
    pair = 2 * SUB
    parts = rows // (2 * pair)
    block = rows // parts
    scale = inverse[...]
    for b in range(parts):
        for row in range(b * block, (b + 1) * block, pair):
            g = row // SUB
            own = jnp.concatenate([
                jnp.broadcast_to(scale[:, g + n : g + n + 1], (SUB, LANES)) for n in range(2)
            ], axis=0)
            for j in range(tiles):
                staged[pl.ds(row, pair), pl.ds(j * LANES, LANES)] = (
                    gated[j, pl.ds(row, pair), :] * own
                ).astype(jnp.bfloat16)
        dense = pl.ds(b * block, block)
        pltpu.make_async_copy(staged.at[dense], out.at[dense], sem).start()
    pltpu.make_async_copy(staged, out, sem).wait()


def body(nsp, ntp, decay_rate, drive_in, gate_in, norm_gain):
    batch, rows, channels = decay_rate.shape
    tiles = channels // LANES
    units = rows // UNIT
    near = spaced(max(SUB, tiles))
    width = -(-(rows // SUB) // LANES) * LANES
    plane = pltpu.VMEM((tiles, rows, LANES), jnp.float32)
    wide = pltpu.VMEM((tiles, -(-(units * APART) // SUB) * SUB + SUB, LANES), jnp.float32)
    half = pltpu.VMEM((rows, channels), jnp.bfloat16)
    outside = pl.BlockSpec(memory_space=pltpu.HBM)
    vmem = pl.BlockSpec(memory_space=pltpu.VMEM)
    gated, inverse = pl.pallas_call(
        functools.partial(kernel, nsp, ntp),
        out_shape=(
            pltpu.VMEM((tiles, rows, LANES), jnp.float32),
            pltpu.VMEM((SUB, width), jnp.float32),
        ),
        in_specs=[outside] * 4,
        out_specs=(vmem, vmem),
        scratch_shapes=[
            pltpu.VMEM((rows, channels), jnp.float32), half, half,
            wide, wide, wide, plane, plane, wide, wide, wide,
            pltpu.VMEM((3, units, tiles * near, LANES), jnp.float32),
            pltpu.VMEM((4, units, SUB * near, LANES), jnp.float32),
            pltpu.VMEM((3, tiles, LANES), jnp.float32),
            pltpu.VMEM((nsp, 3, tiles, LANES), jnp.float32),
            pltpu.VMEM((ntp, SUB, width), jnp.float32),
            pltpu.VMEM((tiles, LANES), jnp.float32),
            pltpu.SemaphoreType.DMA((len(blocked(units)) + 1,)),
            pltpu.SemaphoreType.DMA((3,)),
            pltpu.SemaphoreType.DMA,
        ],
        compiler_params=pltpu.CompilerParams(
            collective_id=0, has_side_effects=True, vmem_limit_bytes=52 * 1024 * 1024
        ),
    )(*(
        pltpu.with_memory_space_constraint(value, pltpu.HBM)
        for value in (
            decay_rate.reshape(rows, channels),
            drive_in.reshape(rows, channels),
            gate_in.reshape(rows, channels),
            norm_gain.reshape(tiles, LANES),
        )
    ))
    result = pl.pallas_call(
        emit,
        out_shape=jax.ShapeDtypeStruct((rows, channels), jnp.bfloat16),
        in_specs=[vmem, vmem],
        out_specs=outside,
        scratch_shapes=[
            pltpu.VMEM((rows, channels), jnp.bfloat16),
            pltpu.SemaphoreType.DMA,
        ],
        compiler_params=pltpu.CompilerParams(vmem_limit_bytes=32 * 1024 * 1024),
    )(
        pltpu.with_memory_space_constraint(gated, pltpu.VMEM),
        pltpu.with_memory_space_constraint(inverse, pltpu.VMEM),
    )
    return result.reshape(batch, rows, channels)


def solution(mesh):
    in_specs = (P(None, "sp", "tp"), P(None, "sp", "tp"), P(None, "sp", "tp"), P("tp"))
    out_specs = P(None, "sp", "tp")
    local = functools.partial(body, mesh.shape["sp"], mesh.shape["tp"])
    return jax.shard_map(local, mesh=mesh, in_specs=in_specs, out_specs=out_specs, check_vma=False)
```

```python
import functools

import jax
import jax.numpy as jnp
from jax import lax
from jax.experimental import pallas as pl
from jax.experimental.pallas import tpu as pltpu
from jax.sharding import PartitionSpec as P

LANES = 128
SUB = 8
LOG2E = 1.4426950408889634
MESH = pl.DeviceIdType.MESH


def spaced(steps):
    return steps + next(more for more in range(4, 40, 4) if (steps + more) % 8 == 4)


PITCH = spaced(SUB)
UNIT = SUB * SUB
APART = SUB * PITCH + 1
PUSH, SIG, LEFT, RIGHT = 2, 1, 1, 8


def joined(early, late):
    (p, f, b), (q, g, c) = early, late
    return p * q, q * f + g, b + p * c


def reduced(spans):
    while len(spans) > 1:
        spans = [joined(*pair) for pair in zip(spans[::2], spans[1::2])] + spans[len(spans) - len(spans) % 2 :]
    return spans[0]


def blocked(units):
    return [range(u, u + 2) for u in range(0, units - 2, 2)] + [range(u, u + 1) for u in range(units - 2 + units % 2, units)]


def kernel(
    nsp, ntp, decay, drive, gate, gain, gated, inverse,
    decay_v, drive_v, gate_v, decay_s, push_s, sig_s, fwd_s, pre_s, base_s, left_s, right_s,
    ends_s, edge_s, enter_s, totals, powers, gain_v, local, trecv, precv,
):
    rows, channels = decay.shape
    tiles = channels // LANES
    units = rows // UNIT
    groups = rows // SUB
    length = rows * nsp
    near = spaced(max(SUB, tiles))
    me, mine = lax.axis_index("sp"), lax.axis_index("tp")
    blocks = blocked(units)
    final = len(blocks) - 1

    def band(block):
        return pl.ds(block[0] * UNIT, len(block) * UNIT)

    def drain(ref, sem):
        pltpu.make_async_copy(ref, ref, sem).wait()

    for n, block in enumerate(blocks):
        pltpu.make_async_copy(decay.at[band(block)], decay_v.at[band(block)], local.at[n]).start()
        pltpu.make_async_copy(
            drive.at[band(block)], drive_v.at[band(block)], local.at[n if n < final else n + 1]
        ).start()

    barrier = pltpu.get_barrier_semaphore()

    def peers():
        ahead_first = (2 * me + 1) // nsp
        for i in range(nsp - 1):
            up = nsp - 1 - i - (i + me + 1) // nsp
            down = i + (nsp - 1 - me + i + 1) // nsp
            yield up * (1 - ahead_first) + down * ahead_first

    for peer in peers():
        pl.semaphore_signal(barrier, inc=1, device_id={"sp": peer}, device_id_type=MESH)
    for d in range(1, ntp):
        pl.semaphore_signal(barrier, inc=1, device_id={"tp": lax.rem(mine + d, ntp)}, device_id_type=MESH)

    zero = jnp.zeros((SUB, LANES), jnp.float32)
    blank = jnp.zeros((tiles, LANES), jnp.float32)

    def at(u, k, shift=0):
        return pl.ds(u * APART + k + shift, SUB, stride=PITCH)

    def spot(g, shift=0):
        return pl.ds(g // SUB * APART + g % SUB * PITCH + shift, SUB)

    def lanes(j):
        return pl.ds(j * LANES if isinstance(j, int) else pl.multiple_of(j * LANES, LANES), LANES)

    def keeps(g, members):
        for j in members:
            decay_s[j, spot(g), :] = jnp.exp2(decay_v[pl.ds(g * SUB, SUB), lanes(j)] * (-LOG2E / length))

    def pushes(g, members):
        for j in members:
            value = drive_v[pl.ds(g * SUB, 2 * SUB), lanes(j)].astype(jnp.float32)
            push_s[j, spot(g, PUSH), :] = value[:SUB]
            push_s[j, spot(g + 1, PUSH), :] = value[SUB:]

    def inside(block):
        return range(block[0] * SUB, (block[-1] + 1) * SUB, 2)

    def scan(block, members):
        spans = {}
        for k in range(SUB):
            for u in block:
                for n, j in enumerate(members):
                    keep = decay_s[j, at(u, k), :]
                    push = push_s[j, at(u, k, PUSH), :]
                    if k == 0:
                        spans[u, n] = keep, push, push
                    else:
                        prod, fwd, bwd = spans[u, n]
                        spans[u, n] = prod * keep, keep * fwd + push, bwd + prod * push
        for (u, n), span in spans.items():
            for q in range(3):
                ends_s[q, u, pl.ds(members[n] * near, SUB), :] = span[q]

    def chunk(u, i):
        return tuple(ends_s[q, u, pl.ds(i, tiles, stride=near), :] for q in range(3))

    whole = []

    def settled(block):
        for u in block:
            whole.append(reduced([chunk(u, i) for i in range(SUB)]))
        whole[:] = [reduced(whole)]

    for n, block in enumerate(blocks):
        if n == final:
            pltpu.make_async_copy(gate, gate_v, local.at[0]).start()
            pltpu.make_async_copy(gain, gain_v, local.at[1]).start()
            drain(decay_v.at[band(block)], local.at[n])
        else:
            drain(fwd_s.at[:, pl.ds(0, len(block) * UNIT * 3 // 2)], local.at[n])
        wide = max(1, min(tiles, SUB // len(block)))
        parts = [range(m, m + wide) for m in range(0, tiles, wide)]
        for members in parts:
            for g in inside(block):
                keeps(g, members)
                keeps(g + 1, members)
                if n < final:
                    pushes(g, members)
            if n > 0 and members is parts[0]:
                settled(blocks[n - 1])
            if n < final:
                scan(block, members)
        if n == final:
            pl.semaphore_wait(barrier, nsp + ntp - 2)
            drain(drive_v.at[band(block)], local.at[n + 1])
            for members in parts:
                for g in inside(block):
                    pushes(g, members)
                scan(block, members)
    settled(blocks[final])

    totals[me, 1], totals[me, 2], totals[me, 0] = whole[0]


    def share(peer, row, kind, sem):
        return pltpu.make_async_remote_copy(
            src_ref=totals.at[me, row],
            dst_ref=totals.at[me, row],
            send_sem=local.at[sem],
            recv_sem=trecv.at[kind],
            device_id={"sp": peer},
            device_id_type=MESH,
        )

    inner = jnp.logical_and(me > 0, me < nsp - 1)
    ways = []
    for peer in peers():
        above = (peer + nsp - me) // nsp
        ways.append((peer, 2 * above, (1 - above) * (me // (nsp - 1))))
    for peer, row, kind in ways:
        share(peer, row, kind, 2).start()

    @pl.when(inner)
    def _():
        for peer, _, kind in ways:
            share(peer, 1, kind, 4).start()

    def counted(count, sem):
        for v in range(nsp):
            if count(v) > 0:

                @pl.when(me == v)
                def _(n=count(v)):
                    drain(fwd_s.at[0, pl.ds(0, n * tiles)], sem)

    def rise(u, carry):
        prod, enter = carry
        for i in range(SUB):
            edge_s[0, u, pl.ds(i * near, tiles), :] = prod
            edge_s[1, u, pl.ds(i * near, tiles), :] = enter
            keep, fwd, _ = chunk(u, i)
            prod, enter = prod * keep, keep * enter + fwd
        return prod, enter

    def fall(n, carry):
        prod, enter = carry
        u = units - 1 - n
        for i in reversed(range(SUB)):
            edge_s[2, u, pl.ds(i * near, tiles), :] = prod
            edge_s[3, u, pl.ds(i * near, tiles), :] = enter
            keep, _, bwd = chunk(u, i)
            prod, enter = prod * keep, keep * enter + bwd
        return prod, enter

    lax.fori_loop(0, units, rise, (blank + 1.0, blank))
    lax.fori_loop(0, units, fall, (blank + 1.0, blank))

    drain(gate_v, local.at[0])

    def edges(q, j):
        return [edge_s[q, u, pl.ds(j, SUB, stride=near), :] for u in range(units)]

    def packed(u, k):
        return pl.ds((u * SUB + k) * SUB, SUB)

    def gates(j, carry):
        for g in range(0, groups, 2):
            value = gate_v[pl.ds(g * SUB, 2 * SUB), lanes(j)].astype(jnp.float32)
            value = 1.0 / (1.0 + jnp.exp2(value * -LOG2E))
            sig_s[j, spot(g, SIG), :] = value[:SUB]
            sig_s[j, spot(g + 1, SIG), :] = value[SUB:]
        pre, fwd = edges(0, j), edges(1, j)
        for k in range(SUB):
            for u in range(units):
                keep = decay_s[j, at(u, k), :]
                fwd[u] = keep * fwd[u] + push_s[j, at(u, k, PUSH), :]
                pre[u] = keep * pre[u]
                fwd_s[j, packed(u, k), :] = fwd[u]
                pre_s[j, packed(u, k), :] = pre[u]
        suf, bwd = edges(2, j), edges(3, j)
        for k in reversed(range(SUB)):
            for u in range(units):
                keep = decay_s[j, at(u, k), :]
                sig = sig_s[j, at(u, k, SIG), :]
                bwd[u] = keep * bwd[u] + push_s[j, at(u, k, PUSH), :]
                suf[u] = keep * suf[u]
                base_s[j, at(u, k), :] = (fwd_s[j, packed(u, k), :] + bwd[u]) * sig
                left_s[j, at(u, k, LEFT), :] = pre_s[j, packed(u, k), :] * sig
                right_s[j, at(u, k, RIGHT), :] = suf[u] * sig
        return carry

    lax.fori_loop(0, tiles, gates, 0)

    def spread(q, j):
        return jnp.broadcast_to(enter_s[q, pl.ds(j, 1), :], (SUB, LANES))

    counted(lambda v: v + max(v - 1, 0) + 2 * max(nsp - 2 - v, 0), trecv.at[0])

    def join(s, enter):
        return totals[s, 1] * enter + totals[s, 2]

    enter_s[0] = lax.fori_loop(1, me, join, jnp.where(me > 0, totals[0, 2], 0.0))

    def settle(j, carry):
        enter = spread(0, j)
        for g in range(groups):
            base_s[j, spot(g), :] = base_s[j, spot(g), :] + left_s[j, spot(g, LEFT), :] * enter
        return carry

    @pl.when(me > 0)
    def _():
        lax.fori_loop(0, tiles, settle, 0)


    def prepend(n, carry):
        enter, span = carry
        e = me + 1 + n
        return enter + span * totals[e, 0], span * totals[e, 1]

    enter, span = lax.fori_loop(0, nsp - 2 - me, prepend, (blank, blank + 1.0))
    enter_s[1] = enter
    enter_s[2] = jnp.where(me < nsp - 1, span, 0.0)
    enters = [(spread(1, j), spread(2, j)) for j in range(tiles)]

    @pl.when(me < nsp - 1)
    def _():
        drain(totals.at[0, 0], trecv.at[1])

    enters = [
        enter + span * jnp.broadcast_to(totals[nsp - 1, 0, pl.ds(j, 1), :], (SUB, LANES))
        for j, (enter, span) in enumerate(enters)
    ]
    width = powers.shape[-1]
    lane = lax.broadcasted_iota(jnp.int32, (SUB, width), 1)
    sums = jnp.zeros((SUB, width), jnp.float32)
    for g in range(groups):
        squares = zero
        for j in range(tiles):
            value = base_s[j, spot(g), :] + right_s[j, spot(g, RIGHT), :] * enters[j]
            squares = squares + value * value
        sums = jnp.where(lane == g, jnp.sum(squares, axis=1, keepdims=True), sums)
    powers[mine] = sums

    tells = []
    for d in sorted(range(1, ntp), key=lambda d: abs(2 * d - ntp)):
        tells.append(pltpu.make_async_remote_copy(
            src_ref=powers.at[mine],
            dst_ref=powers.at[mine],
            send_sem=local.at[3],
            recv_sem=precv,
            device_id={"tp": lax.rem(mine + d, ntp)},
            device_id_type=MESH,
        ))
    for copy in tells:
        copy.start()
    enter_s[1] = enter_s[1] + enter_s[2] * totals[nsp - 1, 0]
    drain(gain_v, local.at[1])

    def weigh(j, carry):
        own = jnp.broadcast_to(gain_v[pl.ds(j, 1), :], (SUB, LANES))
        enter = spread(1, j)
        for g in range(groups):
            value = base_s[j, spot(g), :] + right_s[j, spot(g, RIGHT), :] * enter
            gated[j, pl.ds(g * SUB, SUB), :] = value * own
        return carry

    lax.fori_loop(0, tiles, weigh, 0)

    drain(fwd_s.at[0, pl.ds(0, (nsp - 1) * tiles)], local.at[2])

    @pl.when(inner)
    def _():
        drain(fwd_s.at[0, pl.ds(0, (nsp - 1) * tiles)], local.at[4])

    drain(powers.at[pl.ds(0, ntp - 1)], local.at[3])
    drain(powers.at[pl.ds(0, ntp - 1)], precv)

    power = powers[0]
    for s in range(1, ntp):
        power = power + powers[s]
    power = power * (1.0 / (length * channels * ntp))
    inverse[...] = lax.rsqrt(power + 1e-06) * length ** (-0.5)


def emit(gated, inverse, out, staged, sem):
    rows, channels = out.shape
    tiles = channels // LANES
    pair = 2 * SUB
    cuts = [0, pair, *range(2 * pair, rows + 1, 2 * pair)]
    scale = inverse[...]
    for low, top in zip(cuts, cuts[1:]):
        for row in range(low, top, pair):
            g = row // SUB
            own = jnp.concatenate([
                jnp.broadcast_to(scale[:, g + n : g + n + 1], (SUB, LANES)) for n in range(2)
            ], axis=0)
            for j in range(tiles):
                staged[pl.ds(row, pair), pl.ds(j * LANES, LANES)] = (
                    gated[j, pl.ds(row, pair), :] * own
                ).astype(jnp.bfloat16)
        dense = pl.ds(low, top - low)
        pltpu.make_async_copy(staged.at[dense], out.at[dense], sem).start()
    pltpu.make_async_copy(staged, out, sem).wait()


def body(nsp, ntp, decay_rate, drive_in, gate_in, norm_gain):
    batch, rows, channels = decay_rate.shape
    tiles = channels // LANES
    units = rows // UNIT
    near = spaced(max(SUB, tiles))
    width = -(-(rows // SUB) // LANES) * LANES
    plane = pltpu.VMEM((tiles, rows, LANES), jnp.float32)
    wide = pltpu.VMEM((tiles, -(-(units * APART) // SUB) * SUB + SUB, LANES), jnp.float32)
    half = pltpu.VMEM((rows, channels), jnp.bfloat16)
    outside = pl.BlockSpec(memory_space=pltpu.HBM)
    vmem = pl.BlockSpec(memory_space=pltpu.VMEM)
    gated, inverse = pl.pallas_call(
        functools.partial(kernel, nsp, ntp),
        out_shape=(
            pltpu.VMEM((tiles, rows, LANES), jnp.float32),
            pltpu.VMEM((SUB, width), jnp.float32),
        ),
        in_specs=[outside] * 4,
        out_specs=(vmem, vmem),
        scratch_shapes=[
            pltpu.VMEM((rows, channels), jnp.float32), half, half,
            wide, wide, wide, plane, plane, wide, wide, wide,
            pltpu.VMEM((3, units, tiles * near, LANES), jnp.float32),
            pltpu.VMEM((4, units, SUB * near, LANES), jnp.float32),
            pltpu.VMEM((3, tiles, LANES), jnp.float32),
            pltpu.VMEM((nsp, 3, tiles, LANES), jnp.float32),
            pltpu.VMEM((ntp, SUB, width), jnp.float32),
            pltpu.VMEM((tiles, LANES), jnp.float32),
            pltpu.SemaphoreType.DMA((len(blocked(units)) + 1,)),
            pltpu.SemaphoreType.DMA((2,)),
            pltpu.SemaphoreType.DMA,
        ],
        compiler_params=pltpu.CompilerParams(
            collective_id=0, has_side_effects=True, vmem_limit_bytes=52 * 1024 * 1024
        ),
    )(*(
        pltpu.with_memory_space_constraint(value, pltpu.HBM)
        for value in (
            decay_rate.reshape(rows, channels),
            drive_in.reshape(rows, channels),
            gate_in.reshape(rows, channels),
            norm_gain.reshape(tiles, LANES),
        )
    ))
    result = pl.pallas_call(
        emit,
        out_shape=jax.ShapeDtypeStruct((rows, channels), jnp.bfloat16),
        in_specs=[vmem, vmem],
        out_specs=outside,
        scratch_shapes=[
            pltpu.VMEM((rows, channels), jnp.bfloat16),
            pltpu.SemaphoreType.DMA,
        ],
        compiler_params=pltpu.CompilerParams(vmem_limit_bytes=32 * 1024 * 1024),
    )(
        pltpu.with_memory_space_constraint(gated, pltpu.VMEM),
        pltpu.with_memory_space_constraint(inverse, pltpu.VMEM),
    )
    return result.reshape(batch, rows, channels)


def solution(mesh):
    in_specs = (P(None, "sp", "tp"), P(None, "sp", "tp"), P(None, "sp", "tp"), P("tp"))
    out_specs = P(None, "sp", "tp")
    local = functools.partial(body, mesh.shape["sp"], mesh.shape["tp"])
    return jax.shard_map(local, mesh=mesh, in_specs=in_specs, out_specs=out_specs, check_vma=False)
```

```python
import functools

import jax
import jax.numpy as jnp
from jax import lax
from jax.experimental import pallas as pl
from jax.experimental.pallas import tpu as pltpu
from jax.sharding import PartitionSpec as P

LANES = 128
SUB = 8
LOG2E = 1.4426950408889634
MESH = pl.DeviceIdType.MESH


def spaced(steps):
    return steps + next(more for more in range(4, 40, 4) if (steps + more) % 8 == 4)


PITCH = spaced(SUB)
UNIT = SUB * SUB
APART = SUB * PITCH + 1
PUSH, SIG, LEFT, RIGHT = 2, 1, 1, 8


def joined(early, late):
    (p, f, b), (q, g, c) = early, late
    return p * q, q * f + g, b + p * c


def reduced(spans):
    while len(spans) > 1:
        spans = [joined(*pair) for pair in zip(spans[::2], spans[1::2])] + spans[len(spans) - len(spans) % 2 :]
    return spans[0]


def blocked(units):
    return [range(u, u + 2) for u in range(0, units - 2, 2)] + [range(u, u + 1) for u in range(units - 2 + units % 2, units)]


def kernel(
    nsp, ntp, decay, drive, gate, gain, gated, inverse,
    decay_v, drive_v, gate_v, decay_s, push_s, sig_s, fwd_s, pre_s, base_s, left_s, right_s,
    ends_s, edge_s, enter_s, totals, powers, gain_v, local, trecv, precv,
):
    rows, channels = decay.shape
    tiles = channels // LANES
    units = rows // UNIT
    groups = rows // SUB
    length = rows * nsp
    near = spaced(max(SUB, tiles))
    me, mine = lax.axis_index("sp"), lax.axis_index("tp")
    blocks = blocked(units)
    final = len(blocks) - 1

    def band(block):
        return pl.ds(block[0] * UNIT, len(block) * UNIT)

    def drain(ref, sem):
        pltpu.make_async_copy(ref, ref, sem).wait()

    for n, block in enumerate(blocks):
        pltpu.make_async_copy(decay.at[band(block)], decay_v.at[band(block)], local.at[n]).start()
        pltpu.make_async_copy(
            drive.at[band(block)], drive_v.at[band(block)], local.at[n if n < final else n + 1]
        ).start()

    barrier = pltpu.get_barrier_semaphore()

    def peers():
        ahead_first = (2 * me + 1) // nsp
        for i in range(nsp - 1):
            up = nsp - 1 - i - (i + me + 1) // nsp
            down = i + (nsp - 1 - me + i + 1) // nsp
            yield up * (1 - ahead_first) + down * ahead_first

    for peer in peers():
        pl.semaphore_signal(barrier, inc=1, device_id={"sp": peer}, device_id_type=MESH)
    for d in range(1, ntp):
        pl.semaphore_signal(barrier, inc=1, device_id={"tp": lax.rem(mine + d, ntp)}, device_id_type=MESH)

    zero = jnp.zeros((SUB, LANES), jnp.float32)
    blank = jnp.zeros((tiles, LANES), jnp.float32)

    def at(u, k, shift=0):
        return pl.ds(u * APART + k + shift, SUB, stride=PITCH)

    def spot(g, shift=0):
        return pl.ds(g // SUB * APART + g % SUB * PITCH + shift, SUB)

    def lanes(j):
        return pl.ds(j * LANES if isinstance(j, int) else pl.multiple_of(j * LANES, LANES), LANES)

    def keeps(g, members):
        for j in members:
            decay_s[j, spot(g), :] = jnp.exp2(decay_v[pl.ds(g * SUB, SUB), lanes(j)] * (-LOG2E / length))

    def pushes(g, members):
        for j in members:
            value = drive_v[pl.ds(g * SUB, 2 * SUB), lanes(j)].astype(jnp.float32)
            push_s[j, spot(g, PUSH), :] = value[:SUB]
            push_s[j, spot(g + 1, PUSH), :] = value[SUB:]

    def inside(block):
        return range(block[0] * SUB, (block[-1] + 1) * SUB, 2)

    def scan(block, members):
        spans = {}
        for k in range(SUB):
            for u in block:
                for n, j in enumerate(members):
                    keep = decay_s[j, at(u, k), :]
                    push = push_s[j, at(u, k, PUSH), :]
                    if k == 0:
                        spans[u, n] = keep, push, push
                    else:
                        prod, fwd, bwd = spans[u, n]
                        spans[u, n] = prod * keep, keep * fwd + push, bwd + prod * push
        for (u, n), span in spans.items():
            for q in range(3):
                ends_s[q, u, pl.ds(members[n] * near, SUB), :] = span[q]

    def chunk(u, i):
        return tuple(ends_s[q, u, pl.ds(i, tiles, stride=near), :] for q in range(3))

    whole = []

    def settled(block):
        for u in block:
            whole.append(reduced([chunk(u, i) for i in range(SUB)]))
        whole[:] = [reduced(whole)]

    for n, block in enumerate(blocks):
        if n == final:
            pltpu.make_async_copy(gate, gate_v, local.at[0]).start()
            pltpu.make_async_copy(gain, gain_v, local.at[1]).start()
            drain(decay_v.at[band(block)], local.at[n])
        else:
            drain(fwd_s.at[:, pl.ds(0, len(block) * UNIT * 3 // 2)], local.at[n])
        wide = max(1, min(tiles, SUB // len(block)))
        parts = [range(m, m + wide) for m in range(0, tiles, wide)]
        for members in parts:
            for g in inside(block):
                keeps(g, members)
                keeps(g + 1, members)
                if n < final:
                    pushes(g, members)
            if n > 0 and members is parts[0]:
                settled(blocks[n - 1])
            if n < final:
                scan(block, members)
        if n == final:
            pl.semaphore_wait(barrier, nsp + ntp - 2)
            drain(drive_v.at[band(block)], local.at[n + 1])
            for members in parts:
                for g in inside(block):
                    pushes(g, members)
                scan(block, members)
    settled(blocks[final])

    totals[me, 1], totals[me, 2], totals[me, 0] = whole[0]


    def share(peer, row, kind, sem):
        return pltpu.make_async_remote_copy(
            src_ref=totals.at[me, row],
            dst_ref=totals.at[me, row],
            send_sem=local.at[sem],
            recv_sem=trecv.at[kind],
            device_id={"sp": peer},
            device_id_type=MESH,
        )

    inner = jnp.logical_and(me > 0, me < nsp - 1)
    ways = []
    for peer in peers():
        above = (peer + nsp - me) // nsp
        ways.append((peer, 2 * above, (1 - above) * (me // (nsp - 1))))
    for peer, row, kind in ways:
        share(peer, row, kind, 2).start()

    @pl.when(inner)
    def _():
        for peer, _, kind in ways:
            share(peer, 1, kind, 4).start()

    def counted(count, sem):
        for v in range(nsp):
            if count(v) > 0:

                @pl.when(me == v)
                def _(n=count(v)):
                    drain(fwd_s.at[0, pl.ds(0, n * tiles)], sem)

    def rise(u, carry):
        prod, enter = carry
        for i in range(SUB):
            edge_s[0, u, pl.ds(i * near, tiles), :] = prod
            edge_s[1, u, pl.ds(i * near, tiles), :] = enter
            keep, fwd, _ = chunk(u, i)
            prod, enter = prod * keep, keep * enter + fwd
        return prod, enter

    def fall(n, carry):
        prod, enter = carry
        u = units - 1 - n
        for i in reversed(range(SUB)):
            edge_s[2, u, pl.ds(i * near, tiles), :] = prod
            edge_s[3, u, pl.ds(i * near, tiles), :] = enter
            keep, _, bwd = chunk(u, i)
            prod, enter = prod * keep, keep * enter + bwd
        return prod, enter

    lax.fori_loop(0, units, rise, (blank + 1.0, blank))
    lax.fori_loop(0, units, fall, (blank + 1.0, blank))

    drain(gate_v, local.at[0])

    def edges(q, j):
        return [edge_s[q, u, pl.ds(j, SUB, stride=near), :] for u in range(units)]

    def packed(u, k):
        return pl.ds((u * SUB + k) * SUB, SUB)

    def gates(j, carry):
        for g in range(0, groups, 2):
            value = gate_v[pl.ds(g * SUB, 2 * SUB), lanes(j)].astype(jnp.float32)
            value = 1.0 / (1.0 + jnp.exp2(value * -LOG2E))
            sig_s[j, spot(g, SIG), :] = value[:SUB]
            sig_s[j, spot(g + 1, SIG), :] = value[SUB:]
        pre, fwd = edges(0, j), edges(1, j)
        for k in range(SUB):
            for u in range(units):
                keep = decay_s[j, at(u, k), :]
                fwd[u] = keep * fwd[u] + push_s[j, at(u, k, PUSH), :]
                pre[u] = keep * pre[u]
                fwd_s[j, packed(u, k), :] = fwd[u]
                pre_s[j, packed(u, k), :] = pre[u]
        suf, bwd = edges(2, j), edges(3, j)
        for k in reversed(range(SUB)):
            for u in range(units):
                keep = decay_s[j, at(u, k), :]
                sig = sig_s[j, at(u, k, SIG), :]
                bwd[u] = keep * bwd[u] + push_s[j, at(u, k, PUSH), :]
                suf[u] = keep * suf[u]
                base_s[j, at(u, k), :] = (fwd_s[j, packed(u, k), :] + bwd[u]) * sig
                left_s[j, at(u, k, LEFT), :] = pre_s[j, packed(u, k), :] * sig
                right_s[j, at(u, k, RIGHT), :] = suf[u] * sig
        return carry

    lax.fori_loop(0, tiles, gates, 0)

    def spread(q, j):
        return jnp.broadcast_to(enter_s[q, pl.ds(j, 1), :], (SUB, LANES))

    counted(lambda v: v + max(v - 1, 0) + 2 * max(nsp - 2 - v, 0), trecv.at[0])

    def join(s, enter):
        return totals[s, 1] * enter + totals[s, 2]

    enter_s[0] = lax.fori_loop(1, me, join, jnp.where(me > 0, totals[0, 2], 0.0))

    def settle(j, carry):
        enter = spread(0, j)
        for g in range(groups):
            base_s[j, spot(g), :] = base_s[j, spot(g), :] + left_s[j, spot(g, LEFT), :] * enter
        return carry

    @pl.when(me > 0)
    def _():
        lax.fori_loop(0, tiles, settle, 0)


    def prepend(n, carry):
        enter, span = carry
        e = me + 1 + n
        return enter + span * totals[e, 0], span * totals[e, 1]

    enter, span = lax.fori_loop(0, nsp - 2 - me, prepend, (blank, blank + 1.0))
    enter_s[1] = enter
    enter_s[2] = jnp.where(me < nsp - 1, span, 0.0)
    enters = [(spread(1, j), spread(2, j)) for j in range(tiles)]

    @pl.when(me < nsp - 1)
    def _():
        drain(totals.at[0, 0], trecv.at[1])

    enters = [
        enter + span * jnp.broadcast_to(totals[nsp - 1, 0, pl.ds(j, 1), :], (SUB, LANES))
        for j, (enter, span) in enumerate(enters)
    ]
    width = powers.shape[-1]
    lane = lax.broadcasted_iota(jnp.int32, (SUB, width), 1)
    sums = jnp.zeros((SUB, width), jnp.float32)
    for g in range(groups):
        squares = zero
        for j in range(tiles):
            value = base_s[j, spot(g), :] + right_s[j, spot(g, RIGHT), :] * enters[j]
            squares = squares + value * value
        sums = jnp.where(lane == g, jnp.sum(squares, axis=1, keepdims=True), sums)
    powers[mine] = sums

    tells = []
    for d in sorted(range(1, ntp), key=lambda d: abs(2 * d - ntp)):
        tells.append(pltpu.make_async_remote_copy(
            src_ref=powers.at[mine],
            dst_ref=powers.at[mine],
            send_sem=local.at[3],
            recv_sem=precv,
            device_id={"tp": lax.rem(mine + d, ntp)},
            device_id_type=MESH,
        ))
    for copy in tells:
        copy.start()
    enter_s[1] = enter_s[1] + enter_s[2] * totals[nsp - 1, 0]
    drain(gain_v, local.at[1])

    def weigh(j, carry):
        own = jnp.broadcast_to(gain_v[pl.ds(j, 1), :], (SUB, LANES))
        enter = spread(1, j)
        for g in range(groups):
            value = base_s[j, spot(g), :] + right_s[j, spot(g, RIGHT), :] * enter
            gated[j, pl.ds(g * SUB, SUB), :] = value * own
        return carry

    lax.fori_loop(0, tiles, weigh, 0)

    drain(fwd_s.at[0, pl.ds(0, (nsp - 1) * tiles)], local.at[2])

    @pl.when(inner)
    def _():
        drain(fwd_s.at[0, pl.ds(0, (nsp - 1) * tiles)], local.at[4])

    drain(powers.at[pl.ds(0, ntp - 1)], local.at[3])
    drain(powers.at[pl.ds(0, ntp - 1)], precv)

    power = powers[0]
    for s in range(1, ntp):
        power = power + powers[s]
    power = power * (1.0 / (length * channels * ntp))
    inverse[...] = lax.rsqrt(power + 1e-06) * length ** (-0.5)


def emit(gated, inverse, out, staged, sem):
    rows, channels = out.shape
    tiles = channels // LANES
    pair = 2 * SUB
    cuts = range(0, rows + 1, 4 * pair)
    scale = inverse[...]
    for low, top in zip(cuts, cuts[1:]):
        for row in range(low, top, pair):
            g = row // SUB
            own = jnp.concatenate([
                jnp.broadcast_to(scale[:, g + n : g + n + 1], (SUB, LANES)) for n in range(2)
            ], axis=0)
            for j in range(tiles):
                staged[pl.ds(row, pair), pl.ds(j * LANES, LANES)] = (
                    gated[j, pl.ds(row, pair), :] * own
                ).astype(jnp.bfloat16)
        dense = pl.ds(low, top - low)
        pltpu.make_async_copy(staged.at[dense], out.at[dense], sem).start()
    pltpu.make_async_copy(staged, out, sem).wait()


def body(nsp, ntp, decay_rate, drive_in, gate_in, norm_gain):
    batch, rows, channels = decay_rate.shape
    tiles = channels // LANES
    units = rows // UNIT
    near = spaced(max(SUB, tiles))
    width = -(-(rows // SUB) // LANES) * LANES
    plane = pltpu.VMEM((tiles, rows, LANES), jnp.float32)
    wide = pltpu.VMEM((tiles, -(-(units * APART) // SUB) * SUB + SUB, LANES), jnp.float32)
    half = pltpu.VMEM((rows, channels), jnp.bfloat16)
    outside = pl.BlockSpec(memory_space=pltpu.HBM)
    vmem = pl.BlockSpec(memory_space=pltpu.VMEM)
    gated, inverse = pl.pallas_call(
        functools.partial(kernel, nsp, ntp),
        out_shape=(
            pltpu.VMEM((tiles, rows, LANES), jnp.float32),
            pltpu.VMEM((SUB, width), jnp.float32),
        ),
        in_specs=[outside] * 4,
        out_specs=(vmem, vmem),
        scratch_shapes=[
            pltpu.VMEM((rows, channels), jnp.float32), half, half,
            wide, wide, wide, plane, plane, wide, wide, wide,
            pltpu.VMEM((3, units, tiles * near, LANES), jnp.float32),
            pltpu.VMEM((4, units, SUB * near, LANES), jnp.float32),
            pltpu.VMEM((3, tiles, LANES), jnp.float32),
            pltpu.VMEM((nsp, 3, tiles, LANES), jnp.float32),
            pltpu.VMEM((ntp, SUB, width), jnp.float32),
            pltpu.VMEM((tiles, LANES), jnp.float32),
            pltpu.SemaphoreType.DMA((len(blocked(units)) + 1,)),
            pltpu.SemaphoreType.DMA((2,)),
            pltpu.SemaphoreType.DMA,
        ],
        compiler_params=pltpu.CompilerParams(
            collective_id=0, has_side_effects=True, vmem_limit_bytes=52 * 1024 * 1024
        ),
    )(*(
        pltpu.with_memory_space_constraint(value, pltpu.HBM)
        for value in (
            decay_rate.reshape(rows, channels),
            drive_in.reshape(rows, channels),
            gate_in.reshape(rows, channels),
            norm_gain.reshape(tiles, LANES),
        )
    ))
    result = pl.pallas_call(
        emit,
        out_shape=jax.ShapeDtypeStruct((rows, channels), jnp.bfloat16),
        in_specs=[vmem, vmem],
        out_specs=outside,
        scratch_shapes=[
            pltpu.VMEM((rows, channels), jnp.bfloat16),
            pltpu.SemaphoreType.DMA,
        ],
        compiler_params=pltpu.CompilerParams(vmem_limit_bytes=32 * 1024 * 1024),
    )(
        pltpu.with_memory_space_constraint(gated, pltpu.VMEM),
        pltpu.with_memory_space_constraint(inverse, pltpu.VMEM),
    )
    return result.reshape(batch, rows, channels)


def solution(mesh):
    in_specs = (P(None, "sp", "tp"), P(None, "sp", "tp"), P(None, "sp", "tp"), P("tp"))
    out_specs = P(None, "sp", "tp")
    local = functools.partial(body, mesh.shape["sp"], mesh.shape["tp"])
    return jax.shard_map(local, mesh=mesh, in_specs=in_specs, out_specs=out_specs, check_vma=False)
```
